128 devices in a mesh: dp: 32 (over y, z, core), rep: 4 (over x).
Axes of the slice: x: 4, y: 4, z: 4, core: 2. Of those that a mesh axis runs over, the one named last changes fastest.
Arguments:
- enc: bfloat16 [256, 48, 640], P(('dp', 'rep')), may hold values from -6 to 6
- pred: bfloat16 [256, 17, 640], P(('dp', 'rep')), may hold values from -6 to 6
- labels: int32 [256, 16], P(('dp', 'rep')), may hold values from 1 to 4095
- frame_len: int32 [256], P(('dp', 'rep')), may hold values from 24 to 48, as said below
- label_len: int32 [256], P(('dp', 'rep')), may hold values from 1 to 16, as said below
- w_enc: bfloat16 [640, 640], replicated, may hold values from -0.25 to 0.25
- w_pred: bfloat16 [640, 640], replicated, may hold values from -0.25 to 0.25
- b_joint: bfloat16 [640], replicated, may hold values from -3 to 3
- w_out: bfloat16 [640, 4096], replicated, may hold values from -0.69921875 to 0.69921875
- b_out: bfloat16 [4096], replicated, may hold values from -5 to 5
Outputs:
- step_enc: float32 [640, 640], replicated
- step_pred: float32 [640, 640], replicated
- step_out: float32 [640, 4096], replicated
- step_bias_out: float32 [4096], replicated
- step_bias_joint: float32 [640], replicated
- mean_loss: float32 [], replicated
The draws below stay inside these ranges and needn't reach their ends.
Inputs may be any that keep to these rules, and one draw needn't show every extreme that they name: `frame_len`: the last utterance has all 48 frames. `label_len`: the last utterance has all 16 labels.
All inputs are finite; a program needn't handle non-finite values.
Results may differ from the reference program's by a relative error of at most 0.0055.
Values sent between devices are 32-bit elements; how exact they have to be, the bound alone decides.
A program may use at most 256 MiB of HBM per device.

```python
import jax
import jax.numpy as jnp
from jax import lax

ENC_DIM = 640
PRED_DIM = 640
JOINT = 640
VOCAB = 4096
FRAMES = 48
LABELS = 16
BATCH = 256


def draw_frame_len(key, part):
    positions = jnp.arange(BATCH, dtype=jnp.int32)
    picked = jax.random.randint(jax.random.fold_in(key, 11), (BATCH,), FRAMES // 2, FRAMES + 1)
    return jnp.where(positions == BATCH - 1, FRAMES, picked).astype(jnp.int32)


def draw_label_len(key, part):
    positions = jnp.arange(BATCH, dtype=jnp.int32)
    baseline = LABELS * (BATCH + 2 * positions) // (3 * BATCH)
    jitter = jax.random.randint(jax.random.fold_in(key, 23), (BATCH,), -1, 2)
    lengths = jnp.clip(baseline + jitter, 1, LABELS)
    return jnp.where(positions == BATCH - 1, LABELS, lengths).astype(jnp.int32)


def place_ends(drawn, stream_key, least, top_value):
    place = [jax.random.randint(jax.random.fold_in(stream_key, axis), (), 0, length) for axis, length in enumerate(drawn.shape)]
    main_axis = drawn.shape.index(max(drawn.shape))
    neighbour = place[:main_axis] + [(place[main_axis] + 1) % drawn.shape[main_axis]] + place[main_axis + 1:]
    return drawn.at[tuple(place)].set(least).at[tuple(neighbour)].set(top_value)


def level_of(rng, shape, cuts, smallest, high):
    level = 1.0
    for axis_at, shards_of in cuts:
        steps = jax.random.uniform(jax.random.fold_in(jax.random.fold_in(rng, 6), axis_at), (shards_of,), jnp.float32, smallest / len(cuts), high / len(cuts))
        level = level * jnp.repeat(jnp.exp(steps), shape[axis_at] // shards_of).reshape((-1,) + (1,) * (len(shape) - 1 - axis_at))
    return level


def gaussian(stream_key, shape, width, limit, split=(), held_as=jnp.bfloat16):
    factor_of = level_of(stream_key, shape, split, -0.22, 0.18) if split else 1.0
    result = jax.random.normal(stream_key, shape, jnp.float32) * width * factor_of
    return jnp.minimum(jnp.maximum(result, -limit), limit).astype(held_as)


def setup_inputs(seed: int = 0) -> dict:
    seeds = jax.random.split(jax.random.key(seed), 11)
    return {
        "enc": gaussian(seeds[0], (BATCH, FRAMES, ENC_DIM), 1.0, 6.0, ((0, 128),)),
        "pred": gaussian(seeds[1], (BATCH, LABELS + 1, PRED_DIM), 1.0, 6.0, ((0, 128),)),
        "labels": place_ends(jax.random.randint(seeds[2], (BATCH, LABELS), 1, VOCAB), jax.random.fold_in(seeds[2], 1), 1, VOCAB - 1).astype(jnp.int32),
        "frame_len": draw_frame_len(jax.random.fold_in(seeds[10], 71), 0),
        "label_len": draw_label_len(jax.random.fold_in(seeds[10], 71), 0),
        "w_enc": gaussian(seeds[5], (ENC_DIM, JOINT), ENC_DIM ** -0.5, 0.25),
        "w_pred": gaussian(seeds[6], (PRED_DIM, JOINT), PRED_DIM ** -0.5, 0.25),
        "b_joint": gaussian(seeds[7], (JOINT,), 0.5, 3.0),
        "w_out": gaussian(seeds[8], (JOINT, VOCAB), 0.12, 0.69921875),
        "b_out": gaussian(seeds[9], (VOCAB,), 1.0, 5.0),
    }


NEG = -1e+30
EPS = 1e-06

def forward_rows(blank, emit):
    count_labels = blank.shape[1]
    positions = jnp.arange(count_labels, dtype=jnp.int32)

    def along_labels(carry_left, inputs):
        top_term, emit_here = inputs
        cell_value = jnp.logaddexp(top_term, carry_left)
        return (cell_value + emit_here, cell_value)

    def along_frames(top_row, inputs):
        blank_row, emit_row = inputs
        unused_carry, alpha_row = lax.scan(along_labels, jnp.float32(NEG), (top_row, emit_row))
        return (alpha_row + blank_row, alpha_row)
    first_top = jnp.where(positions == 0, 0.0, NEG).astype(jnp.float32)
    unused_last, alpha = lax.scan(along_frames, first_top, (blank, emit))
    return alpha

def backward_rows(blank, emit, frame_count, label_count):
    num_frames, count_labels = blank.shape
    positions = jnp.arange(count_labels, dtype=jnp.int32)
    neg_row = jnp.full((count_labels,), NEG, jnp.float32)
    terminal = jnp.where(positions == label_count, 0.0, NEG).astype(jnp.float32)

    def along_labels_back(carry_right, inputs):
        below_value, blank_here, emit_here, live = inputs
        cell_value = jnp.logaddexp(below_value + blank_here, carry_right + emit_here)
        cell_value = jnp.where(live, cell_value, NEG).astype(jnp.float32)
        return (cell_value, cell_value)

    def along_frames_back(carry_below, inputs):
        frame_pos, blank_row, emit_row = inputs
        below = jnp.where(frame_pos == frame_count - 1, terminal, jnp.where(frame_pos >= frame_count, neg_row, carry_below))
        live = (positions <= label_count) & (frame_pos < frame_count)
        unused_carry, beta_row = lax.scan(along_labels_back, jnp.float32(NEG), (below, blank_row, emit_row, live), reverse=True)
        return (beta_row, (beta_row, below))
    frame_ids = jnp.arange(num_frames, dtype=jnp.int32)
    unused_last, (beta, below) = lax.scan(along_frames_back, neg_row, (frame_ids, blank, emit), reverse=True)
    return (beta, below)

def utterance_terms(enc_row, pred_row, label_row, frame_count, label_count, w_enc, w_pred, b_joint, w_out, b_out):
    num_frames = enc_row.shape[0]
    count_labels = pred_row.shape[0]
    joint_width = w_enc.shape[1]
    vocab_size = w_out.shape[1]
    enc_proj = jnp.dot(enc_row, w_enc, preferred_element_type=jnp.float32)
    pred_proj = jnp.dot(pred_row, w_pred, preferred_element_type=jnp.float32) + b_joint.astype(jnp.float32)
    hidden = jnp.tanh(enc_proj[:, None, :] + pred_proj[None, :, :]).astype(jnp.bfloat16)
    hidden = lax.optimization_barrier(hidden.reshape(num_frames * count_labels, joint_width))
    logits = jnp.dot(hidden, w_out, preferred_element_type=jnp.float32) + b_out.astype(jnp.float32)
    log_probs = jax.nn.log_softmax(logits, axis=-1)
    targets = jnp.concatenate([label_row.astype(jnp.int32), jnp.ones((1,), jnp.int32)])
    target_cols = jnp.tile(targets, num_frames)
    vocab_pos = jnp.arange(vocab_size, dtype=jnp.int32)
    is_target = vocab_pos[None, :] == target_cols[:, None]
    emit = lax.optimization_barrier(jnp.sum(jnp.where(is_target, log_probs, 0.0), axis=1)).reshape(num_frames, count_labels)
    blank = log_probs[:, 0].reshape(num_frames, count_labels)
    alpha = forward_rows(blank, emit)
    beta, below = backward_rows(blank, emit, frame_count, label_count)
    log_total = beta[0, 0]
    right = jnp.concatenate([beta[:, 1:], jnp.full((num_frames, 1), NEG, jnp.float32)], axis=1)
    blank_occ = jnp.exp(alpha + blank + below - log_total).reshape(-1)
    emit_occ = jnp.exp(alpha + emit + right - log_total).reshape(-1)
    probs = jnp.exp(log_probs)
    grad_logits = probs * (blank_occ + emit_occ)[:, None]
    grad_logits = grad_logits - jnp.where(vocab_pos[None, :] == 0, blank_occ[:, None], 0.0)
    grad_logits = grad_logits - jnp.where(is_target, emit_occ[:, None], 0.0)
    grad_logits = lax.optimization_barrier(grad_logits.astype(jnp.bfloat16))
    grad_out = lax.dot_general(hidden, grad_logits, (((0,), (0,)), ((), ())), preferred_element_type=jnp.float32)
    grad_bias_out = lax.optimization_barrier(jnp.sum(grad_logits.astype(jnp.float32), axis=0))
    grad_hidden = lax.dot_general(grad_logits, w_out, (((1,), (1,)), ((), ())), preferred_element_type=jnp.float32)
    hidden_wide = hidden.astype(jnp.float32)
    grad_pre = (grad_hidden * (1.0 - hidden_wide * hidden_wide)).reshape(num_frames, count_labels, joint_width)
    grad_enc_proj = lax.optimization_barrier(lax.optimization_barrier(jnp.sum(grad_pre, axis=1)).astype(jnp.bfloat16))
    grad_pred_proj = lax.optimization_barrier(lax.optimization_barrier(jnp.sum(grad_pre, axis=0)).astype(jnp.bfloat16))
    grad_enc = lax.dot_general(enc_row, grad_enc_proj, (((0,), (0,)), ((), ())), preferred_element_type=jnp.float32)
    grad_pred = lax.dot_general(pred_row, grad_pred_proj, (((0,), (0,)), ((), ())), preferred_element_type=jnp.float32)
    grad_bias_joint = lax.optimization_barrier(jnp.sum(grad_pred_proj.astype(jnp.float32), axis=0))
    return (-log_total, (grad_enc, grad_pred, grad_out, grad_bias_out, grad_bias_joint))

def local_sums(enc, pred, labels, frame_len, label_len, w_enc, w_pred, b_joint, w_out, b_out):
    initial = (jnp.zeros(w_enc.shape, jnp.float32), jnp.zeros(w_pred.shape, jnp.float32), jnp.zeros(w_out.shape, jnp.float32), jnp.zeros(b_out.shape, jnp.float32), jnp.zeros(b_joint.shape, jnp.float32))

    def one_utterance(carry, inputs):
        loss_sum, grad_sums = carry
        enc_row, pred_row, label_row, frame_count, label_count = inputs
        loss_one, grads_one = utterance_terms(enc_row, pred_row, label_row, frame_count, label_count, w_enc, w_pred, b_joint, w_out, b_out)
        added = tuple((total + term for total, term in zip(grad_sums, grads_one)))
        return ((loss_sum + loss_one, added), None)
    (loss_sum, grads), unused_ys = lax.scan(one_utterance, (jnp.float32(0.0), initial), (enc, pred, labels, frame_len, label_len))
    return (loss_sum, grads)

def reference(enc, pred, labels, frame_len, label_len, w_enc, w_pred, b_joint, w_out, b_out):
    loss_sum, grads = local_sums(enc, pred, labels, frame_len, label_len, w_enc, w_pred, b_joint, w_out, b_out)
    param_count = sum((int(item.size) for item in grads))
    total_sq = jnp.float32(0.0)
    for item in grads:
        total_sq = total_sq + jnp.sum(item * item)
    scale = lax.rsqrt(total_sq / jnp.float32(param_count) + EPS)
    label_total = jnp.sum(label_len).astype(jnp.float32)
    return (grads[0] * scale, grads[1] * scale, grads[2] * scale, grads[3] * scale, grads[4] * scale, loss_sum / label_total)
```

```python
import functools

import jax
import jax.numpy as jnp
from jax import lax
from jax.experimental import pallas as pl
from jax.experimental.pallas import tpu as pltpu
from jax.sharding import PartitionSpec as P

AXES = ("dp", "rep")
NEG = -1e30
EPS = 1e-06
F32 = jnp.float32
BF16 = jnp.bfloat16
LANES = 128
SLOT = 32
CHUNK = 512
ROWS = 416


def local_kernel(
    labels_ref, frame_ref, label_ref, enc_ref, pred_ref, w_enc_ref, w_pred_ref, b_joint_ref, w_out_ref, b_out_ref,
    g_out_ref, g_side_ref,
    hid, hid_t, logits, dhid, dlog, top, tot, lse, occ, emit_occ, blank_occ, target, blank_d, emit_d, alpha_d,
    beta_d, below_d, right_d, pred_pad, dpred_pad, denc, g_buf, bias_acc, sems,
):
    utts, frames, _ = enc_ref.shape
    slots = pred_ref.shape[1]
    width = w_enc_ref.shape[1]
    vocab = w_out_ref.shape[1]
    rows_all = hid.shape[0]
    cells = utts * slots * frames
    diags = frames + slots - 1
    blocks = [(i, u, (i * slots + u) * frames, SLOT * i + u) for i in range(utts) for u in range(slots)]
    lane_row = lax.broadcasted_iota(jnp.int32, (1, LANES), 1)
    lane_cell = lax.broadcasted_iota(jnp.int32, (frames, LANES), 1)

    def label_at(i, u):
        return labels_ref[i, u] if u < slots - 1 else 1

    pred_pad[...] = jnp.zeros_like(pred_pad)
    hid[cells:, :] = jnp.zeros((rows_all - cells, width), BF16)
    enc_proj = [jnp.dot(enc_ref[i], w_enc_ref[...], preferred_element_type=F32) for i in range(utts)]
    for i in range(utts):
        pred_pad[SLOT * i : SLOT * i + slots, :] = pred_ref[i]
    pred_proj = jnp.dot(pred_pad[...], w_pred_ref[...], preferred_element_type=F32) + b_joint_ref[...].astype(F32)
    for i, u, row, col in blocks:
        hid[row : row + frames, :] = jnp.tanh(enc_proj[i] + pred_proj[col : col + 1, :]).astype(BF16)
    hid_t[...] = hid[...].T

    label_row = jnp.full((1, LANES), -1, jnp.int32)
    for i, u, row, col in blocks:
        label_row = jnp.where(lane_row == col, label_at(i, u), label_row)
    picks = lax.broadcasted_iota(jnp.int32, (vocab, LANES), 0) == label_row
    picks = picks.astype(F32).astype(BF16)
    w_pick = jnp.dot(w_out_ref[...], picks, preferred_element_type=F32).astype(BF16)
    b_pick = jnp.dot(
        jnp.broadcast_to(b_out_ref[...], (16, vocab)), picks, preferred_element_type=F32
    )[:1, :]
    w_blank = jnp.broadcast_to(w_out_ref[:, :1].astype(F32), (width, LANES)).astype(BF16)
    w_two = jnp.concatenate([w_pick, w_blank], axis=1)
    b_blank = b_out_ref[:, :1].astype(F32)

    top[...] = jnp.full_like(top, NEG)
    tot[...] = jnp.zeros_like(tot)

    def forward(c, carry):
        cols = pl.ds(pl.multiple_of(c * CHUNK, CHUNK), CHUNK)
        w_c = w_out_ref[:, cols]
        b_c = b_out_ref[:, cols].astype(F32)
        for r in range(0, rows_all, ROWS):
            z = jnp.dot(hid[r : r + ROWS, :], w_c, preferred_element_type=F32) + b_c
            logits[r : r + ROWS, cols] = z
            tiles = [z[:, k : k + LANES] for k in range(0, CHUNK, LANES)]
            old = top[r : r + ROWS, :]
            new = functools.reduce(jnp.maximum, tiles, old)
            top[r : r + ROWS, :] = new
            tot[r : r + ROWS, :] = tot[r : r + ROWS, :] * jnp.exp(old - new) + sum(jnp.exp(t - new) for t in tiles)
        return carry

    lax.fori_loop(0, vocab // CHUNK, forward, 0)

    for r in range(0, rows_all, ROWS):
        row_top = jnp.max(top[r : r + ROWS, :], axis=1, keepdims=True)
        row_sum = jnp.sum(tot[r : r + ROWS, :] * jnp.exp(top[r : r + ROWS, :] - row_top), axis=1, keepdims=True)
        row_lse = jnp.broadcast_to(row_top + jnp.log(row_sum), (ROWS, LANES))
        lse[r : r + ROWS, :] = row_lse
        two = jnp.dot(hid[r : r + ROWS, :], w_two, preferred_element_type=F32)
        top[r : r + ROWS, :] = two[:, :LANES] + b_pick - row_lse
        tot[r : r + ROWS, :] = two[:, LANES:] + b_blank - row_lse

    blank_d[...] = jnp.full_like(blank_d, NEG)
    emit_d[...] = jnp.full_like(emit_d, NEG)
    for i, u, row, col in blocks:
        here = lane_cell == col
        emit_d[u : u + frames, :] = jnp.where(here, top[row : row + frames, :], emit_d[u : u + frames, :])
        blank_d[u : u + frames, :] = jnp.where(here, tot[row : row + frames, :], blank_d[u : u + frames, :])
    label_pos = lax.rem(lane_row, SLOT)
    frame_count = jnp.full((1, LANES), 0, jnp.int32)
    label_count = jnp.full((1, LANES), -1, jnp.int32)
    for i in range(utts):
        mine = lane_row // SLOT == i
        frame_count = jnp.where(mine, frame_ref[i], frame_count)
        label_count = jnp.where(mine, label_ref[i], label_count)

    def join(a, b):
        hi = jnp.maximum(a, b)
        return hi + jnp.log(1.0 + jnp.exp(jnp.minimum(a, b) - hi))

    alpha = jnp.where((label_pos == 0) & (lane_row < SLOT * utts), 0.0, NEG).astype(F32)
    beta = jnp.full((1, LANES), NEG, F32)
    alpha_d[0:1, :] = alpha
    for step in range(diags):
        d = diags - 1 - step
        t = d - label_pos
        live = (t >= 0) & (t < frame_count) & (label_pos <= label_count)
        last = (t == frame_count - 1) & (label_pos == label_count)
        below = jnp.where(last, 0.0, beta)
        right = pltpu.roll(beta, LANES - 1, 1)
        below_d[d : d + 1, :] = below
        right_d[d : d + 1, :] = right
        beta = jnp.where(live, join(below + blank_d[d : d + 1, :], right + emit_d[d : d + 1, :]), NEG)
        beta_d[d : d + 1, :] = beta
        if step > 0:
            left = pltpu.roll(alpha + emit_d[step - 1 : step, :], 1, 1)
            alpha = join(alpha + blank_d[step - 1 : step, :], left)
            alpha_d[step : step + 1, :] = alpha
    total = jnp.full((1, LANES), 0.0, F32)
    for i in range(utts):
        beta_0 = jnp.sum(jnp.where(lane_row == SLOT * i, beta, 0.0), axis=1, keepdims=True)
        total = jnp.where(lane_row // SLOT == i, beta_0, total)
    span = slice(0, diags)
    blank_d[span, :] = jnp.exp(
        jnp.minimum(alpha_d[span, :] + blank_d[span, :] + below_d[span, :] - total, 80.0)
    )
    emit_d[span, :] = jnp.exp(jnp.minimum(alpha_d[span, :] + emit_d[span, :] + right_d[span, :] - total, 80.0))

    pad = slice(cells, rows_all)
    occ[pad, :] = jnp.zeros((rows_all - cells, LANES), F32)
    emit_occ[pad, :] = jnp.zeros((rows_all - cells, LANES), F32)
    blank_occ[pad, :] = jnp.zeros((rows_all - cells, LANES), F32)
    target[pad, :] = jnp.full((rows_all - cells, LANES), -1, jnp.int32)
    for i, u, row, col in blocks:
        here = slice(row, row + frames)
        b = jnp.broadcast_to(blank_d[u : u + frames, col : col + 1], (frames, LANES))
        e = jnp.broadcast_to(emit_d[u : u + frames, col : col + 1], (frames, LANES))
        blank_occ[here, :] = b
        emit_occ[here, :] = e
        occ[here, :] = b + e
        target[here, :] = jnp.full((frames, LANES), label_at(i, u), jnp.int32)

    dhid[...] = jnp.zeros_like(dhid)

    def out_copy(c, slot):
        cols = pl.ds(pl.multiple_of(c * CHUNK, CHUNK), CHUNK)
        return pltpu.make_async_copy(g_buf.at[slot], g_out_ref.at[:, cols], sems.at[slot])

    def backward(c, carry):
        cols = pl.ds(pl.multiple_of(c * CHUNK, CHUNK), CHUNK)
        slot = lax.rem(c, 2)
        w_c = w_out_ref[:, cols]
        first = c == 0
        for r in range(0, rows_all, ROWS):
            here = slice(r, r + ROWS)
            row_lse, row_occ, row_emit = lse[here, :], occ[here, :], emit_occ[here, :]
            row_target = target[here, :] - c * CHUNK
            lane = lax.broadcasted_iota(jnp.int32, (ROWS, LANES), 1)
            for k in range(0, CHUNK, LANES):
                z = logits[here, pl.ds(pl.multiple_of(c * CHUNK + k, LANES), LANES)]
                d = jnp.exp(z - row_lse) * row_occ - jnp.where(lane + k == row_target, row_emit, 0.0)
                if k == 0:
                    d = d - jnp.where((lane == 0) & first, blank_occ[here, :], 0.0)
                dlog[here, k : k + LANES] = d.astype(BF16)
            dhid[here, :] += lax.dot_general(
                dlog[here, :], w_c, (((1,), (1,)), ((), ())), preferred_element_type=F32
            )

        @pl.when(c >= 2)
        def _():
            out_copy(c - 2, slot).wait()

        g_buf[slot] = jnp.dot(hid_t[...], dlog[...], preferred_element_type=F32)
        bias_acc[:, cols] = jnp.dot(jnp.ones((16, rows_all), BF16), dlog[...], preferred_element_type=F32)[:8, :]
        out_copy(c, slot).start()
        return carry

    steps = vocab // CHUNK
    lax.fori_loop(0, steps, backward, 0)

    dpred_pad[...] = jnp.zeros_like(dpred_pad)
    for i in range(utts):
        enc_sum = jnp.zeros((frames, width), F32)
        for u in range(slots):
            row = (i * slots + u) * frames
            h = hid[row : row + frames, :].astype(F32)
            dpre = dhid[row : row + frames, :] * (1.0 - h * h)
            enc_sum = enc_sum + dpre
            dpred_pad[SLOT * i + u : SLOT * i + u + 1, :] = jnp.sum(dpre, axis=0, keepdims=True)
        denc[i] = enc_sum.astype(BF16)
    dpred = dpred_pad[...].astype(BF16)
    over_rows = (((0,), (0,)), ((), ()))
    g_enc = jnp.zeros((width, width), F32)
    for i in range(utts):
        g_enc = g_enc + lax.dot_general(enc_ref[i], denc[i], over_rows, preferred_element_type=F32)
    g_side_ref[0:width, :] = g_enc
    g_side_ref[width : 2 * width, :] = lax.dot_general(pred_pad[...], dpred, over_rows, preferred_element_type=F32)
    at = 2 * width
    g_side_ref[at:, :] = jnp.zeros((g_side_ref.shape[0] - at, width), F32)
    g_side_ref[at : at + 1, :] = jnp.sum(dpred.astype(F32), axis=0, keepdims=True)
    for k in range(0, vocab, width):
        n = min(width, vocab - k)
        at += 1
        g_side_ref[at : at + 1, 0:n] = bias_acc[0:1, k : k + n]
    head = (lax.rem(lane_row, SLOT) == 0) & (lane_row < SLOT * utts)
    g_side_ref[at + 1 : at + 2, 0:LANES] = jnp.where(head, -beta_d[0:1, :], 0.0)
    g_side_ref[at + 2 : at + 3, 0:LANES] = jnp.where(head, label_count.astype(F32), 0.0)
    for c in range(max(0, steps - 2), steps):
        out_copy(c, c % 2).wait()


def side_rows(width, vocab):
    return 2 * width + 1 + -(-vocab // width) + 2


def local_grads(enc, pred, labels, frame_len, label_len, w_enc, w_pred, b_joint, w_out, b_out):
    utts, frames, enc_dim = enc.shape
    slots, pred_dim = pred.shape[1:]
    width, vocab = w_out.shape
    rows_all = -(-utts * slots * frames // ROWS) * ROWS
    diags = frames + slots
    diag_rows = -(-diags // 8) * 8
    n_side = -(-side_rows(width, vocab) // 16) * 16
    smem = pl.BlockSpec(memory_space=pltpu.SMEM)
    vmem = pl.BlockSpec(memory_space=pltpu.VMEM)
    cell = lambda t: pltpu.VMEM((rows_all, LANES), t)
    diag = pltpu.VMEM((diag_rows, LANES), F32)
    return pl.pallas_call(
        local_kernel,
        out_shape=(jax.ShapeDtypeStruct((width, vocab), F32), jax.ShapeDtypeStruct((n_side, width), F32)),
        in_specs=[smem] * 3 + [vmem] * 7,
        out_specs=(pl.BlockSpec(memory_space=pl.ANY), vmem),
        scratch_shapes=[
            pltpu.VMEM((rows_all, width), BF16),
            pltpu.VMEM((width, rows_all), BF16),
            pltpu.VMEM((rows_all, vocab), F32),
            pltpu.VMEM((rows_all, width), F32),
            pltpu.VMEM((rows_all, CHUNK), BF16),
            cell(F32), cell(F32), cell(F32), cell(F32), cell(F32), cell(F32), cell(jnp.int32),
            diag, diag, diag, diag, diag, diag,
            pltpu.VMEM((SLOT * utts, pred_dim), BF16),
            pltpu.VMEM((SLOT * utts, width), F32),
            pltpu.VMEM((utts, frames, width), BF16),
            pltpu.VMEM((2, width, CHUNK), F32),
            pltpu.VMEM((8, vocab), F32),
            pltpu.SemaphoreType.DMA((2,)),
        ],
        compiler_params=pltpu.CompilerParams(vmem_limit_bytes=66_000_000),
        name="local_grads",
    )(labels, frame_len, label_len, enc, pred, w_enc, w_pred, b_joint.reshape(1, width), w_out, b_out.reshape(1, vocab))


def per_device(enc, pred, labels, frame_len, label_len, w_enc, w_pred, b_joint, w_out, b_out):
    width, vocab = w_out.shape
    g_out, g_side = local_grads(enc, pred, labels, frame_len, label_len, w_enc, w_pred, b_joint, w_out, b_out)
    g_out, g_side = lax.psum((g_out, g_side), AXES)
    at = 2 * width
    bias_rows = -(-vocab // width)
    grads = g_side[: at + 1 + bias_rows, :]
    squares = jnp.sum(g_out * g_out) + jnp.sum(grads * grads)
    count = w_enc.size + w_pred.size + w_out.size + b_out.size + b_joint.size
    scale = lax.rsqrt(squares / jnp.float32(count) + EPS)
    g_side_scaled = grads * scale
    bias_out = g_side_scaled[at + 1 :, :].reshape(-1)[:vocab]
    loss_sum, label_sum = jnp.sum(g_side[at + 1 + bias_rows : at + 3 + bias_rows, :LANES], axis=1)
    return (
        g_side_scaled[:width],
        g_side_scaled[width:at],
        g_out * scale,
        bias_out,
        g_side_scaled[at],
        loss_sum / label_sum,
    )


def solution(mesh):
    split = P(AXES)
    in_specs = (split, split, split, split, split, P(), P(), P(), P(), P())
    return jax.shard_map(per_device, mesh=mesh, in_specs=in_specs, out_specs=(P(),) * 6, check_vma=False)
```

```python
import functools

import jax
import jax.numpy as jnp
from jax import lax
from jax.experimental import pallas as pl
from jax.experimental.pallas import tpu as pltpu
from jax.sharding import PartitionSpec as P

AXES = ("dp", "rep")
NEG = -1e30
EPS = 1e-06
F32 = jnp.float32
BF16 = jnp.bfloat16
LANES = 128
SLOT = 32
CHUNK = 512
ROWS = 416


def local_kernel(
    labels_ref, frame_ref, label_ref, enc_ref, pred_ref, w_enc_ref, w_pred_ref, b_joint_ref, w_out_ref, b_out_ref,
    grads_ref,
    hid, hid_t, logits, dhid, dlog, top, tot, lse, occ, emit_occ, blank_occ, target, blank_d, emit_d, alpha_d,
    beta_d, below_d, right_d, pred_pad, dpred_pad, denc, g_buf, bias_acc, g_side, tail, sems, side_sems,
):
    utts, frames, _ = enc_ref.shape
    slots = pred_ref.shape[1]
    width = w_enc_ref.shape[1]
    vocab = w_out_ref.shape[1]
    rows_all = hid.shape[0]
    cells = utts * slots * frames
    diags = frames + slots - 1
    blocks = [(i, u, (i * slots + u) * frames, SLOT * i + u) for i in range(utts) for u in range(slots)]
    lane_row = lax.broadcasted_iota(jnp.int32, (1, LANES), 1)
    lane_cell = lax.broadcasted_iota(jnp.int32, (frames, LANES), 1)

    def label_at(i, u):
        return labels_ref[i, u] if u < slots - 1 else 1

    pred_pad[...] = jnp.zeros_like(pred_pad)
    hid[cells:, :] = jnp.zeros((rows_all - cells, width), BF16)
    enc_proj = [jnp.dot(enc_ref[i], w_enc_ref[...], preferred_element_type=F32) for i in range(utts)]
    for i in range(utts):
        pred_pad[SLOT * i : SLOT * i + slots, :] = pred_ref[i]
    pred_proj = jnp.dot(pred_pad[...], w_pred_ref[...], preferred_element_type=F32) + b_joint_ref[...].astype(F32)
    for i, u, row, col in blocks:
        hid[row : row + frames, :] = jnp.tanh(enc_proj[i] + pred_proj[col : col + 1, :]).astype(BF16)
    hid_t[...] = hid[...].T

    label_row = jnp.full((1, LANES), -1, jnp.int32)
    for i, u, row, col in blocks:
        label_row = jnp.where(lane_row == col, label_at(i, u), label_row)
    picks = lax.broadcasted_iota(jnp.int32, (vocab, LANES), 0) == label_row
    picks = picks.astype(F32).astype(BF16)
    w_pick = jnp.dot(w_out_ref[...], picks, preferred_element_type=F32).astype(BF16)
    b_pick = jnp.dot(
        jnp.broadcast_to(b_out_ref[...], (16, vocab)), picks, preferred_element_type=F32
    )[:1, :]
    w_blank = jnp.broadcast_to(w_out_ref[:, :1].astype(F32), (width, LANES)).astype(BF16)
    w_two = jnp.concatenate([w_pick, w_blank], axis=1)
    b_blank = b_out_ref[:, :1].astype(F32)

    top[...] = jnp.full_like(top, NEG)
    tot[...] = jnp.zeros_like(tot)

    def forward(c, carry):
        cols = pl.ds(pl.multiple_of(c * CHUNK, CHUNK), CHUNK)
        w_c = w_out_ref[:, cols]
        b_c = b_out_ref[:, cols].astype(F32)
        for r in range(0, rows_all, ROWS):
            z = jnp.dot(hid[r : r + ROWS, :], w_c, preferred_element_type=F32) + b_c
            logits[r : r + ROWS, cols] = z
            tiles = [z[:, k : k + LANES] for k in range(0, CHUNK, LANES)]
            old = top[r : r + ROWS, :]
            new = functools.reduce(jnp.maximum, tiles, old)
            top[r : r + ROWS, :] = new
            tot[r : r + ROWS, :] = tot[r : r + ROWS, :] * jnp.exp(old - new) + sum(jnp.exp(t - new) for t in tiles)
        return carry

    lax.fori_loop(0, vocab // CHUNK, forward, 0)

    for r in range(0, rows_all, ROWS):
        row_top = jnp.max(top[r : r + ROWS, :], axis=1, keepdims=True)
        row_sum = jnp.sum(tot[r : r + ROWS, :] * jnp.exp(top[r : r + ROWS, :] - row_top), axis=1, keepdims=True)
        row_lse = jnp.broadcast_to(row_top + jnp.log(row_sum), (ROWS, LANES))
        lse[r : r + ROWS, :] = row_lse
        two = jnp.dot(hid[r : r + ROWS, :], w_two, preferred_element_type=F32)
        top[r : r + ROWS, :] = two[:, :LANES] + b_pick - row_lse
        tot[r : r + ROWS, :] = two[:, LANES:] + b_blank - row_lse

    blank_d[...] = jnp.full_like(blank_d, NEG)
    emit_d[...] = jnp.full_like(emit_d, NEG)
    for i, u, row, col in blocks:
        here = lane_cell == col
        emit_d[u : u + frames, :] = jnp.where(here, top[row : row + frames, :], emit_d[u : u + frames, :])
        blank_d[u : u + frames, :] = jnp.where(here, tot[row : row + frames, :], blank_d[u : u + frames, :])
    label_pos = lax.rem(lane_row, SLOT)
    frame_count = jnp.full((1, LANES), 0, jnp.int32)
    label_count = jnp.full((1, LANES), -1, jnp.int32)
    for i in range(utts):
        mine = lane_row // SLOT == i
        frame_count = jnp.where(mine, frame_ref[i], frame_count)
        label_count = jnp.where(mine, label_ref[i], label_count)

    def join(a, b):
        hi = jnp.maximum(a, b)
        return hi + jnp.log(1.0 + jnp.exp(jnp.minimum(a, b) - hi))

    alpha = jnp.where((label_pos == 0) & (lane_row < SLOT * utts), 0.0, NEG).astype(F32)
    beta = jnp.full((1, LANES), NEG, F32)
    alpha_d[0:1, :] = alpha
    for step in range(diags):
        d = diags - 1 - step
        t = d - label_pos
        live = (t >= 0) & (t < frame_count) & (label_pos <= label_count)
        last = (t == frame_count - 1) & (label_pos == label_count)
        below = jnp.where(last, 0.0, beta)
        right = pltpu.roll(beta, LANES - 1, 1)
        below_d[d : d + 1, :] = below
        right_d[d : d + 1, :] = right
        beta = jnp.where(live, join(below + blank_d[d : d + 1, :], right + emit_d[d : d + 1, :]), NEG)
        beta_d[d : d + 1, :] = beta
        if step > 0:
            left = pltpu.roll(alpha + emit_d[step - 1 : step, :], 1, 1)
            alpha = join(alpha + blank_d[step - 1 : step, :], left)
            alpha_d[step : step + 1, :] = alpha
    total = jnp.full((1, LANES), 0.0, F32)
    for i in range(utts):
        beta_0 = jnp.sum(jnp.where(lane_row == SLOT * i, beta, 0.0), axis=1, keepdims=True)
        total = jnp.where(lane_row // SLOT == i, beta_0, total)
    span = slice(0, diags)
    blank_d[span, :] = jnp.exp(
        jnp.minimum(alpha_d[span, :] + blank_d[span, :] + below_d[span, :] - total, 80.0)
    )
    emit_d[span, :] = jnp.exp(jnp.minimum(alpha_d[span, :] + emit_d[span, :] + right_d[span, :] - total, 80.0))

    pad = slice(cells, rows_all)
    occ[pad, :] = jnp.zeros((rows_all - cells, LANES), F32)
    emit_occ[pad, :] = jnp.zeros((rows_all - cells, LANES), F32)
    blank_occ[pad, :] = jnp.zeros((rows_all - cells, LANES), F32)
    target[pad, :] = jnp.full((rows_all - cells, LANES), -1, jnp.int32)
    for i, u, row, col in blocks:
        here = slice(row, row + frames)
        b = jnp.broadcast_to(blank_d[u : u + frames, col : col + 1], (frames, LANES))
        e = jnp.broadcast_to(emit_d[u : u + frames, col : col + 1], (frames, LANES))
        blank_occ[here, :] = b
        emit_occ[here, :] = e
        occ[here, :] = b + e
        target[here, :] = jnp.full((frames, LANES), label_at(i, u), jnp.int32)

    dhid[...] = jnp.zeros_like(dhid)

    def out_copies(c, slot):
        return [
            pltpu.make_async_copy(
                g_buf.at[slot, :, pl.ds(k * LANES, LANES)],
                grads_ref.at[pl.ds(pl.multiple_of((c * (CHUNK // LANES) + k) * width, 8), width), :],
                sems.at[slot, k],
            )
            for k in range(CHUNK // LANES)
        ]

    def backward(c, carry):
        cols = pl.ds(pl.multiple_of(c * CHUNK, CHUNK), CHUNK)
        slot = lax.rem(c, 2)
        w_c = w_out_ref[:, cols]
        first = c == 0
        for r in range(0, rows_all, ROWS):
            here = slice(r, r + ROWS)
            row_lse, row_occ, row_emit = lse[here, :], occ[here, :], emit_occ[here, :]
            row_target = target[here, :] - c * CHUNK
            lane = lax.broadcasted_iota(jnp.int32, (ROWS, LANES), 1)
            for k in range(0, CHUNK, LANES):
                z = logits[here, pl.ds(pl.multiple_of(c * CHUNK + k, LANES), LANES)]
                d = jnp.exp(z - row_lse) * row_occ - jnp.where(lane + k == row_target, row_emit, 0.0)
                if k == 0:
                    d = d - jnp.where((lane == 0) & first, blank_occ[here, :], 0.0)
                dlog[here, k : k + LANES] = d.astype(BF16)
            dhid[here, :] += lax.dot_general(
                dlog[here, :], w_c, (((1,), (1,)), ((), ())), preferred_element_type=F32
            )

        @pl.when(c >= 2)
        def _():
            for copy in out_copies(c - 2, slot):
                copy.wait()

        g_buf[slot] = jnp.dot(hid_t[...], dlog[...], preferred_element_type=F32)
        bias_acc[:, cols] = jnp.dot(jnp.ones((16, rows_all), BF16), dlog[...], preferred_element_type=F32)[:8, :]
        for copy in out_copies(c, slot):
            copy.start()
        return carry

    steps = vocab // CHUNK
    lax.fori_loop(0, steps, backward, 0)

    dpred_pad[...] = jnp.zeros_like(dpred_pad)
    for i in range(utts):
        enc_sum = jnp.zeros((frames, width), F32)
        for u in range(slots):
            row = (i * slots + u) * frames
            h = hid[row : row + frames, :].astype(F32)
            dpre = dhid[row : row + frames, :] * (1.0 - h * h)
            enc_sum = enc_sum + dpre
            dpred_pad[SLOT * i + u : SLOT * i + u + 1, :] = jnp.sum(dpre, axis=0, keepdims=True)
        denc[i] = enc_sum.astype(BF16)
    dpred = dpred_pad[...].astype(BF16)
    over_rows = (((0,), (0,)), ((), ()))
    g_enc = jnp.zeros((width, width), F32)
    for i in range(utts):
        g_enc = g_enc + lax.dot_general(enc_ref[i], denc[i], over_rows, preferred_element_type=F32)
    g_side[0:width, :] = g_enc
    g_side[width : 2 * width, :] = lax.dot_general(pred_pad[...], dpred, over_rows, preferred_element_type=F32)
    at = 2 * width
    g_side[at:, :] = jnp.zeros((g_side.shape[0] - at, width), F32)
    g_side[at : at + 1, :] = jnp.sum(dpred.astype(F32), axis=0, keepdims=True)
    for k in range(0, vocab, width):
        n = min(width, vocab - k)
        at += 1
        g_side[at : at + 1, 0:n] = bias_acc[0:1, k : k + n]
    tail[...] = jnp.zeros_like(tail)
    head = (lax.rem(lane_row, SLOT) == 0) & (lane_row < SLOT * utts)
    tail[0:1, :] = jnp.where(head, -beta_d[0:1, :], 0.0)
    tail[1:2, :] = jnp.where(head, label_count.astype(F32), 0.0)
    first = vocab // LANES * width
    n_side = g_side.shape[0]
    last_copies = [
        pltpu.make_async_copy(
            g_side.at[:, pl.ds(k * LANES, LANES)], grads_ref.at[pl.ds(first + k * n_side, n_side), :], side_sems.at[k]
        )
        for k in range(width // LANES)
    ]
    first += width // LANES * n_side
    last_copies.append(
        pltpu.make_async_copy(tail, grads_ref.at[pl.ds(first, tail.shape[0]), :], side_sems.at[width // LANES])
    )
    for copy in last_copies:
        copy.start()
    for c in range(max(0, steps - 2), steps):
        for copy in out_copies(c, c % 2):
            copy.wait()
    for copy in last_copies:
        copy.wait()


UNIT = 512


def layout(width, vocab):
    n_side = -(-(2 * width + 1 + -(-vocab // width)) // 8) * 8
    used = vocab // LANES * width + width // LANES * n_side
    units = -(-(used + 8) // (2 * UNIT))
    parts = [(units + 5 - p) // 6 * UNIT for p in range(6)]
    return n_side, used, parts


def local_grads(enc, pred, labels, frame_len, label_len, w_enc, w_pred, b_joint, w_out, b_out):
    utts, frames, enc_dim = enc.shape
    slots, pred_dim = pred.shape[1:]
    width, vocab = w_out.shape
    rows_all = -(-utts * slots * frames // ROWS) * ROWS
    diags = frames + slots
    diag_rows = -(-diags // 8) * 8
    n_side, used, parts = layout(width, vocab)
    n_rows = 2 * sum(parts)
    smem = pl.BlockSpec(memory_space=pltpu.SMEM)
    vmem = pl.BlockSpec(memory_space=pltpu.VMEM)
    cell = lambda t: pltpu.VMEM((rows_all, LANES), t)
    diag = pltpu.VMEM((diag_rows, LANES), F32)
    return pl.pallas_call(
        local_kernel,
        out_shape=jax.ShapeDtypeStruct((n_rows, LANES), F32),
        in_specs=[smem] * 3 + [vmem] * 7,
        out_specs=pl.BlockSpec(memory_space=pl.ANY),
        scratch_shapes=[
            pltpu.VMEM((rows_all, width), BF16),
            pltpu.VMEM((width, rows_all), BF16),
            pltpu.VMEM((rows_all, vocab), F32),
            pltpu.VMEM((rows_all, width), F32),
            pltpu.VMEM((rows_all, CHUNK), BF16),
            cell(F32), cell(F32), cell(F32), cell(F32), cell(F32), cell(F32), cell(jnp.int32),
            diag, diag, diag, diag, diag, diag,
            pltpu.VMEM((SLOT * utts, pred_dim), BF16),
            pltpu.VMEM((SLOT * utts, width), F32),
            pltpu.VMEM((utts, frames, width), BF16),
            pltpu.VMEM((2, width, CHUNK), F32),
            pltpu.VMEM((8, vocab), F32),
            pltpu.VMEM((n_side, width), F32),
            pltpu.VMEM((n_rows - used, LANES), F32),
            pltpu.SemaphoreType.DMA((2, CHUNK // LANES)),
            pltpu.SemaphoreType.DMA((width // LANES + 1,)),
        ],
        compiler_params=pltpu.CompilerParams(vmem_limit_bytes=66_000_000),
        name="local_grads",
    )(labels, frame_len, label_len, enc, pred, w_enc, w_pred, b_joint.reshape(1, width), w_out, b_out.reshape(1, vocab))


def exchange_kernel(parts, used, grads_ref, full, squares_ref, data, from_core, arrived, local_sems, send_sems, recv_sems):
    dp, x = lax.axis_index("dp"), lax.axis_index("rep")
    core = lax.rem(dp, 2)
    z = lax.rem(dp // 2, 4)
    y = dp // 8
    place = (x, y, z)
    half_rows = sum(parts)
    mine, theirs = core * half_rows, (1 - core) * half_rows
    bases = [sum(parts[:p]) for p in range(6)]

    def device(x, y, z, core):
        return ((y * 4 + z) * 2 + core, x)

    other_core = device(x, y, z, 1 - core)

    def link(p, s):
        axis = (p + s) % 3
        v = place[axis]
        second = lax.rem((p + s) // 3 + core, 2)
        peer = second * (3 - v) + (1 - second) * (v + 1 - 2 * lax.rem(v, 2))
        bit = second * (v // 2) + (1 - second) * lax.rem((v + 1) // 2, 2)
        where = list(place)
        where[axis] = peer
        return device(*where, core), bit

    barrier = pltpu.get_barrier_semaphore()
    peers = [other_core] + [link(p, 0)[0] for p in range(6)]
    for peer in peers:
        pl.semaphore_signal(barrier, inc=1, device_id=peer, device_id_type=pl.DeviceIdType.MESH)
    pl.semaphore_wait(barrier, len(peers))

    def rows(start, n):
        return pl.ds(pl.multiple_of(start, 8), n)

    def send(src, dst, index, peer):
        copy = pltpu.make_async_remote_copy(
            src_ref=src, dst_ref=dst, send_sem=send_sems.at[index], recv_sem=recv_sems.at[index],
            device_id=peer, device_id_type=pl.DeviceIdType.MESH,
        )
        copy.start()
        return copy

    sent = []
    local, swapped = [], []
    for p in range(6):
        here = pl.ds(bases[p], parts[p])
        swapped.append(
            send(grads_ref.at[rows(theirs + bases[p], parts[p]), :], from_core.at[here, :], p, other_core)
        )
        copy = pltpu.make_async_copy(
            grads_ref.at[rows(mine + bases[p], parts[p]), :], data.at[here, :], local_sems.at[p]
        )
        copy.start()
        local.append(copy)
    sent += swapped

    offset = list(bases)
    slots = [0] * 6
    landing = {}
    at = 0
    for p in range(6):
        for s in range(6):
            landing[p, s] = at
            at += parts[p] >> (s + 1)
    steps = {}

    def start_reduce(p, s):
        peer, bit = link(p, s)
        n = parts[p] >> (s + 1)
        steps[p, s] = send(
            data.at[rows(offset[p] + (1 - bit) * n, n), :], arrived.at[pl.ds(landing[p, s], n), :], 6 + 6 * s + p, peer
        )
        offset[p] = offset[p] + bit * n
        sent.append(steps[p, s])

    def finish_reduce(p, s):
        n = parts[p] >> (s + 1)
        steps[p, s].wait_recv()
        here = rows(offset[p], n)
        total = data[here, :] + arrived[pl.ds(landing[p, s], n), :]
        if s < 5:
            data[here, :] = total
        else:
            full[rows(mine + offset[p], n), :] = total

    for s in range(6):
        for p in range(6):
            if s == 0:
                local[p].wait()
                swapped[p].wait_recv()
                here = pl.ds(bases[p], parts[p])
                data[here, :] += from_core[here, :]
            else:
                finish_reduce(p, s - 1)
            if p > 0:
                start_reduce(p - 1, s)
        start_reduce(5, s)

    gathers = {}

    def start_gather(p, s):
        peer, bit = link(p, s)
        n = parts[p] >> (s + 1)
        here = full.at[rows(mine + offset[p], n), :]
        gathers[p, s] = send(here, here, 42 + 6 * s + p, peer)
        sent.append(gathers[p, s])
        if s == 0:
            give_core(p, offset[p], n, 0)
            other = bases[p] + (1 - bit) * n
            gathers[p, "other"] = other
        offset[p] = offset[p] - bit * n

    crossed = []

    def give_core(p, start, n, which):
        here = full.at[rows(mine + start, n), :]
        copy = send(here, here, 78 + 2 * p + which, other_core)
        crossed.append(copy)
        sent.append(copy)

    for s in range(5, -1, -1):
        for p in range(6):
            if s == 5:
                finish_reduce(p, 5)
                if p > 0:
                    start_gather(p - 1, s)
            else:
                gathers[p, s + 1].wait_recv()
                start_gather(p, s)
        if s == 5:
            start_gather(5, s)
    for p in range(6):
        gathers[p, 0].wait_recv()
        give_core(p, gathers[p, "other"], parts[p] >> 1, 1)
    for copy in crossed:
        copy.wait_recv()

    block, lines = 960, 64

    def add_squares(k, total):
        here = full[rows(k * block, block), :].reshape(block // lines, lines, LANES)
        return total + jnp.sum(here * here, axis=0)

    whole = used // block
    total = lax.fori_loop(0, whole, add_squares, jnp.zeros((lines, LANES), F32))
    total = jnp.sum(total.reshape(lines // 8, 8, LANES), axis=0)
    rest = full[whole * block : used, :].reshape(-1, 8, LANES)
    squares_ref[...] = total + jnp.sum(rest * rest, axis=0)
    for copy in sent:
        copy.wait_send()


def exchange(grads, width, vocab):
    _, used, parts = layout(width, vocab)
    half_rows = sum(parts)
    landed = sum(parts[p] >> (s + 1) for p in range(6) for s in range(6))
    vmem = pl.BlockSpec(memory_space=pltpu.VMEM)
    return pl.pallas_call(
        functools.partial(exchange_kernel, parts, used),
        out_shape=(jax.ShapeDtypeStruct(grads.shape, F32), jax.ShapeDtypeStruct((8, LANES), F32)),
        in_specs=[pl.BlockSpec(memory_space=pl.ANY)],
        out_specs=(vmem, vmem),
        scratch_shapes=[
            pltpu.VMEM((half_rows, LANES), F32),
            pltpu.VMEM((half_rows, LANES), F32),
            pltpu.VMEM((landed, LANES), F32),
            pltpu.SemaphoreType.DMA((6,)),
            pltpu.SemaphoreType.DMA((90,)),
            pltpu.SemaphoreType.DMA((90,)),
        ],
        compiler_params=pltpu.CompilerParams(collective_id=0, has_side_effects=True, vmem_limit_bytes=44_000_000),
        name="exchange",
    )(grads)


def finish_kernel(n_side, used, count, full, squares_ref, out_ref, enc_ref, pred_ref, bias_ref, joint_ref, loss_ref, buf, side_buf, sems):
    width, vocab = out_ref.shape
    squares = jnp.sum(jnp.sum(squares_ref[...], axis=0, keepdims=True), axis=1, keepdims=True)
    scale = lax.rsqrt(squares * (1.0 / count) + EPS)
    copies = []
    steps = vocab // CHUNK
    per = CHUNK // LANES
    for c in range(steps):
        slot = c % buf.shape[0]
        if c >= buf.shape[0]:
            copies[c - buf.shape[0]].wait()
        for k in range(per):
            v = c * per + k
            buf[slot, :, k * LANES : (k + 1) * LANES] = full[v * width : (v + 1) * width, :] * scale
        copy = pltpu.make_async_copy(buf.at[slot], out_ref.at[:, pl.ds(c * CHUNK, CHUNK)], sems.at[slot])
        copy.start()
        copies.append(copy)
    first = vocab // LANES * width
    side_copies = []
    for i, ref in enumerate((enc_ref, pred_ref)):
        for k in range(width // LANES):
            row = first + k * n_side + i * width
            side_buf[i, :, k * LANES : (k + 1) * LANES] = full[row : row + width, :] * scale
        copy = pltpu.make_async_copy(side_buf.at[i], ref, sems.at[buf.shape[0] + i])
        copy.start()
        side_copies.append(copy)
    for k in range(width // LANES):
        row = first + k * n_side + 2 * width
        joint_ref[:, k * LANES : (k + 1) * LANES] = full[row : row + 1, :] * scale
        for r in range(-(-vocab // width)):
            lane = r * width + k * LANES
            if lane < vocab:
                bias_ref[:, lane : lane + LANES] = full[row + 1 + r : row + 2 + r, :] * scale
    loss = jnp.sum(full[used : used + 1, :], axis=1, keepdims=True)
    labels = jnp.sum(full[used + 1 : used + 2, :], axis=1, keepdims=True)
    loss_ref[...] = jnp.broadcast_to(loss / labels, loss_ref.shape)
    for copy in copies[-buf.shape[0] :] + side_copies:
        copy.wait()


def finish(full, squares, width, vocab, count):
    n_side, used, _ = layout(width, vocab)
    vmem = pl.BlockSpec(memory_space=pltpu.VMEM)
    anywhere = pl.BlockSpec(memory_space=pl.ANY)
    shape = jax.ShapeDtypeStruct
    return pl.pallas_call(
        functools.partial(finish_kernel, n_side, used, float(count)),
        out_shape=(
            shape((width, vocab), F32), shape((width, width), F32), shape((width, width), F32),
            shape((1, vocab), F32), shape((1, width), F32), shape((1, LANES), F32),
        ),
        in_specs=[vmem, vmem],
        out_specs=(anywhere, anywhere, anywhere, vmem, vmem, vmem),
        scratch_shapes=[
            pltpu.VMEM((4, width, CHUNK), F32),
            pltpu.VMEM((2, width, width), F32),
            pltpu.SemaphoreType.DMA((6,)),
        ],
        compiler_params=pltpu.CompilerParams(vmem_limit_bytes=40_000_000),
        name="finish",
    )(full, squares)


def per_device(enc, pred, labels, frame_len, label_len, w_enc, w_pred, b_joint, w_out, b_out):
    width, vocab = w_out.shape
    grads = local_grads(enc, pred, labels, frame_len, label_len, w_enc, w_pred, b_joint, w_out, b_out)
    full, squares = exchange(grads, width, vocab)
    count = w_enc.size + w_pred.size + w_out.size + b_out.size + b_joint.size
    out, g_enc, g_pred, bias, joint, loss = finish(full, squares, width, vocab, count)
    return g_enc, g_pred, out, bias.reshape(vocab), joint.reshape(width), loss[0, 0]


def solution(mesh):
    split = P(AXES)
    in_specs = (split, split, split, split, split, P(), P(), P(), P(), P())
    return jax.shard_map(per_device, mesh=mesh, in_specs=in_specs, out_specs=(P(),) * 6, check_vma=False)
```

```python
import functools

import jax
import jax.numpy as jnp
from jax import lax
from jax.experimental import pallas as pl
from jax.experimental.pallas import tpu as pltpu
from jax.sharding import PartitionSpec as P

AXES = ("dp", "rep")
NEG = -1e30
EPS = 1e-06
F32 = jnp.float32
BF16 = jnp.bfloat16
LANES = 128
SLOT = 32
CHUNK = 512
ROWS = 416


def local_kernel(
    labels_ref, frame_ref, label_ref, enc_ref, pred_ref, w_enc_ref, w_pred_ref, b_joint_ref, w_out_hbm, b_out_ref,
    side_ref, dlog_ref, hid_t_ref,
    hid, hid_t, logits, dhid, dlog, top, tot, lse, occ, emit_occ, blank_occ, target, blank_d, emit_d, alpha_d,
    beta_d, below_d, right_d, pred_pad, dpred_pad, denc, bias_acc, slabs, tail, w_out_ref, sems, side_sems, load_sem, hid_sem,
):
    utts, frames, _ = enc_ref.shape
    slots = pred_ref.shape[1]
    width = w_enc_ref.shape[1]
    vocab = w_out_ref.shape[1]
    rows_all = hid.shape[0]
    load = pltpu.make_async_copy(w_out_hbm, w_out_ref, load_sem)
    load.start()
    cells = utts * slots * frames
    diags = frames + slots - 1
    blocks = [(i, u, (i * slots + u) * frames, SLOT * i + u) for i in range(utts) for u in range(slots)]
    lane_row = lax.broadcasted_iota(jnp.int32, (1, LANES), 1)
    lane_cell = lax.broadcasted_iota(jnp.int32, (frames, LANES), 1)

    def label_at(i, u):
        return labels_ref[i, u] if u < slots - 1 else 1

    pred_pad[...] = jnp.zeros_like(pred_pad)
    hid[cells:, :] = jnp.zeros((rows_all - cells, width), BF16)
    enc_proj = [jnp.dot(enc_ref[i], w_enc_ref[...], preferred_element_type=F32) for i in range(utts)]
    for i in range(utts):
        pred_pad[SLOT * i : SLOT * i + slots, :] = pred_ref[i]
    pred_proj = jnp.dot(pred_pad[...], w_pred_ref[...], preferred_element_type=F32) + b_joint_ref[...].astype(F32)
    for i, u, row, col in blocks:
        hid[row : row + frames, :] = jnp.tanh(enc_proj[i] + pred_proj[col : col + 1, :]).astype(BF16)
    hid_t[...] = hid[...].T
    hid_copy = pltpu.make_async_copy(hid_t, hid_t_ref, hid_sem)
    hid_copy.start()
    load.wait()

    label_row = jnp.full((1, LANES), -1, jnp.int32)
    for i, u, row, col in blocks:
        label_row = jnp.where(lane_row == col, label_at(i, u), label_row)
    picks = lax.broadcasted_iota(jnp.int32, (vocab, LANES), 0) == label_row
    picks = picks.astype(F32).astype(BF16)
    w_pick = jnp.dot(w_out_ref[...], picks, preferred_element_type=F32).astype(BF16)
    b_pick = jnp.dot(
        jnp.broadcast_to(b_out_ref[...], (16, vocab)), picks, preferred_element_type=F32
    )[:1, :]
    w_blank = jnp.broadcast_to(w_out_ref[:, :1].astype(F32), (width, LANES)).astype(BF16)
    w_two = jnp.concatenate([w_pick, w_blank], axis=1)
    b_blank = b_out_ref[:, :1].astype(F32)

    top[...] = jnp.full_like(top, NEG)
    tot[...] = jnp.zeros_like(tot)

    def forward(c, carry):
        cols = pl.ds(pl.multiple_of(c * CHUNK, CHUNK), CHUNK)
        w_c = w_out_ref[:, cols]
        b_c = b_out_ref[:, cols].astype(F32)
        for r in range(0, rows_all, ROWS):
            z = jnp.dot(hid[r : r + ROWS, :], w_c, preferred_element_type=F32) + b_c
            logits[r : r + ROWS, cols] = z
            tiles = [z[:, k : k + LANES] for k in range(0, CHUNK, LANES)]
            old = top[r : r + ROWS, :]
            new = functools.reduce(jnp.maximum, tiles, old)
            top[r : r + ROWS, :] = new
            tot[r : r + ROWS, :] = tot[r : r + ROWS, :] * jnp.exp(old - new) + sum(jnp.exp(t - new) for t in tiles)
        return carry

    lax.fori_loop(0, vocab // CHUNK, forward, 0)

    for r in range(0, rows_all, ROWS):
        row_top = jnp.max(top[r : r + ROWS, :], axis=1, keepdims=True)
        row_sum = jnp.sum(tot[r : r + ROWS, :] * jnp.exp(top[r : r + ROWS, :] - row_top), axis=1, keepdims=True)
        row_lse = jnp.broadcast_to(row_top + jnp.log(row_sum), (ROWS, LANES))
        lse[r : r + ROWS, :] = row_lse
        two = jnp.dot(hid[r : r + ROWS, :], w_two, preferred_element_type=F32)
        top[r : r + ROWS, :] = two[:, :LANES] + b_pick - row_lse
        tot[r : r + ROWS, :] = two[:, LANES:] + b_blank - row_lse

    blank_d[...] = jnp.full_like(blank_d, NEG)
    emit_d[...] = jnp.full_like(emit_d, NEG)
    for i, u, row, col in blocks:
        here = lane_cell == col
        emit_d[u : u + frames, :] = jnp.where(here, top[row : row + frames, :], emit_d[u : u + frames, :])
        blank_d[u : u + frames, :] = jnp.where(here, tot[row : row + frames, :], blank_d[u : u + frames, :])
    label_pos = lax.rem(lane_row, SLOT)
    frame_count = jnp.full((1, LANES), 0, jnp.int32)
    label_count = jnp.full((1, LANES), -1, jnp.int32)
    for i in range(utts):
        mine = lane_row // SLOT == i
        frame_count = jnp.where(mine, frame_ref[i], frame_count)
        label_count = jnp.where(mine, label_ref[i], label_count)

    def join(a, b):
        hi = jnp.maximum(a, b)
        return hi + jnp.log(1.0 + jnp.exp(jnp.minimum(a, b) - hi))

    alpha = jnp.where((label_pos == 0) & (lane_row < SLOT * utts), 0.0, NEG).astype(F32)
    beta = jnp.full((1, LANES), NEG, F32)
    alpha_d[0:1, :] = alpha
    for step in range(diags):
        d = diags - 1 - step
        t = d - label_pos
        live = (t >= 0) & (t < frame_count) & (label_pos <= label_count)
        last = (t == frame_count - 1) & (label_pos == label_count)
        below = jnp.where(last, 0.0, beta)
        right = pltpu.roll(beta, LANES - 1, 1)
        below_d[d : d + 1, :] = below
        right_d[d : d + 1, :] = right
        beta = jnp.where(live, join(below + blank_d[d : d + 1, :], right + emit_d[d : d + 1, :]), NEG)
        beta_d[d : d + 1, :] = beta
        if step > 0:
            left = pltpu.roll(alpha + emit_d[step - 1 : step, :], 1, 1)
            alpha = join(alpha + blank_d[step - 1 : step, :], left)
            alpha_d[step : step + 1, :] = alpha
    total = jnp.full((1, LANES), 0.0, F32)
    for i in range(utts):
        beta_0 = jnp.sum(jnp.where(lane_row == SLOT * i, beta, 0.0), axis=1, keepdims=True)
        total = jnp.where(lane_row // SLOT == i, beta_0, total)
    span = slice(0, diags)
    blank_d[span, :] = jnp.exp(
        jnp.minimum(alpha_d[span, :] + blank_d[span, :] + below_d[span, :] - total, 80.0)
    )
    emit_d[span, :] = jnp.exp(jnp.minimum(alpha_d[span, :] + emit_d[span, :] + right_d[span, :] - total, 80.0))

    pad = slice(cells, rows_all)
    occ[pad, :] = jnp.zeros((rows_all - cells, LANES), F32)
    emit_occ[pad, :] = jnp.zeros((rows_all - cells, LANES), F32)
    blank_occ[pad, :] = jnp.zeros((rows_all - cells, LANES), F32)
    target[pad, :] = jnp.full((rows_all - cells, LANES), -1, jnp.int32)
    for i, u, row, col in blocks:
        here = slice(row, row + frames)
        b = jnp.broadcast_to(blank_d[u : u + frames, col : col + 1], (frames, LANES))
        e = jnp.broadcast_to(emit_d[u : u + frames, col : col + 1], (frames, LANES))
        blank_occ[here, :] = b
        emit_occ[here, :] = e
        occ[here, :] = b + e
        target[here, :] = jnp.full((frames, LANES), label_at(i, u), jnp.int32)

    dhid[...] = jnp.zeros_like(dhid)

    bias_acc[...] = jnp.zeros_like(bias_acc)

    def out_copy(c, slot):
        cols = pl.ds(pl.multiple_of(c * CHUNK, CHUNK), CHUNK)
        return pltpu.make_async_copy(dlog.at[slot], dlog_ref.at[:, cols], sems.at[slot])

    def backward(c, carry):
        cols = pl.ds(pl.multiple_of(c * CHUNK, CHUNK), CHUNK)
        slot = lax.rem(c, 2)
        w_c = w_out_ref[:, cols]
        first = c == 0

        @pl.when(c >= 2)
        def _():
            out_copy(c - 2, slot).wait()

        sums = [jnp.zeros((8, LANES), F32)] * (CHUNK // LANES)
        for r in range(0, rows_all, ROWS):
            here = slice(r, r + ROWS)
            row_lse, row_occ, row_emit = lse[here, :], occ[here, :], emit_occ[here, :]
            row_target = target[here, :] - c * CHUNK
            lane = lax.broadcasted_iota(jnp.int32, (ROWS, LANES), 1)
            parts = []
            for k in range(0, CHUNK, LANES):
                z = logits[here, pl.ds(pl.multiple_of(c * CHUNK + k, LANES), LANES)]
                d = jnp.exp(z - row_lse) * row_occ - jnp.where(lane + k == row_target, row_emit, 0.0)
                if k == 0:
                    d = d - jnp.where((lane == 0) & first, blank_occ[here, :], 0.0)
                sums[k // LANES] = sums[k // LANES] + jnp.sum(d.reshape(ROWS // 8, 8, LANES), axis=0)
                parts.append(d.astype(BF16))
            d = jnp.concatenate(parts, axis=1)
            dlog[slot, here, :] = d
            dhid[here, :] += lax.dot_general(d, w_c, (((1,), (1,)), ((), ())), preferred_element_type=F32)
        bias_acc[:, cols] = jnp.concatenate(sums, axis=1)
        out_copy(c, slot).start()
        return carry

    steps = vocab // CHUNK
    lax.fori_loop(0, steps, backward, 0)

    dpred_pad[...] = jnp.zeros_like(dpred_pad)
    for i in range(utts):
        enc_sum = jnp.zeros((frames, width), F32)
        for u in range(slots):
            row = (i * slots + u) * frames
            h = hid[row : row + frames, :].astype(F32)
            dpre = dhid[row : row + frames, :] * (1.0 - h * h)
            enc_sum = enc_sum + dpre
            dpred_pad[SLOT * i + u : SLOT * i + u + 1, :] = jnp.sum(dpre, axis=0, keepdims=True)
        denc[i] = enc_sum.astype(BF16)
    dpred = dpred_pad[...].astype(BF16)
    over_rows = (((0,), (0,)), ((), ()))
    g_enc = jnp.zeros((width, width), F32)
    for i in range(utts):
        g_enc = g_enc + lax.dot_general(enc_ref[i], denc[i], over_rows, preferred_element_type=F32)
    g_pred = lax.dot_general(pred_pad[...], dpred, over_rows, preferred_element_type=F32)
    per = width // LANES
    last_copies = []
    for i, g in enumerate((g_enc, g_pred)):
        for k in range(per):
            slabs[i, k] = g[:, k * LANES : (k + 1) * LANES]
        for k in range(per):
            last_copies.append(
                pltpu.make_async_copy(slabs.at[i, k], side_ref.at[i, pl.ds(k * width, width), :], side_sems.at[i, k])
            )
            last_copies[-1].start()
    tail[...] = jnp.zeros_like(tail)
    bias = jnp.sum(bias_acc[...], axis=0, keepdims=True)
    joint = jnp.sum(dpred.astype(F32), axis=0, keepdims=True)
    for k in range(vocab // LANES):
        tail[0, k : k + 1, :] = bias[:, k * LANES : (k + 1) * LANES]
    for k in range(per):
        tail[0, vocab // LANES + k : vocab // LANES + k + 1, :] = joint[:, k * LANES : (k + 1) * LANES]
    head = (lax.rem(lane_row, SLOT) == 0) & (lane_row < SLOT * utts)
    tail[1, 0:1, :] = jnp.where(head, -beta_d[0:1, :], 0.0)
    tail[1, 1:2, :] = jnp.where(head, label_count.astype(F32), 0.0)
    for i in range(2):
        last_copies.append(
            pltpu.make_async_copy(
                tail.at[i], side_ref.at[i, pl.ds(per * width, tail.shape[1]), :], side_sems.at[i, per]
            )
        )
        last_copies[-1].start()
    for c in range(max(0, steps - 2), steps):
        out_copy(c, c % 2).wait()
    hid_copy.wait()
    for copy in last_copies:
        copy.wait()


UNIT = 512
PER_CHUNK = 5
BLOCK = 1024
GAP = 2
EXTRA = 2


def layout(width, vocab):
    chunks = 1 + vocab // BLOCK
    main = PER_CHUNK * UNIT
    half = chunks * main + EXTRA * UNIT
    per = width // LANES
    assert main == 4 * width and BLOCK == 8 * LANES and per == 5
    return chunks, main, half


def local_grads(enc, pred, labels, frame_len, label_len, w_enc, w_pred, b_joint, w_out, b_out):
    utts, frames, enc_dim = enc.shape
    slots, pred_dim = pred.shape[1:]
    width, vocab = w_out.shape
    rows_all = -(-utts * slots * frames // ROWS) * ROWS
    diags = frames + slots
    diag_rows = -(-diags // 8) * 8
    chunks, main, half = layout(width, vocab)
    side_rows = main + EXTRA * UNIT
    shape = jax.ShapeDtypeStruct
    smem = pl.BlockSpec(memory_space=pltpu.SMEM)
    vmem = pl.BlockSpec(memory_space=pltpu.VMEM)
    anywhere = pl.BlockSpec(memory_space=pl.ANY)
    cell = lambda t: pltpu.VMEM((rows_all, LANES), t)
    diag = pltpu.VMEM((diag_rows, LANES), F32)
    return pl.pallas_call(
        local_kernel,
        out_shape=(
            shape((2, side_rows, LANES), F32), shape((rows_all, vocab), BF16), shape((width, rows_all), BF16),
        ),
        in_specs=[smem] * 3 + [vmem] * 5 + [anywhere, vmem],
        out_specs=(anywhere,) * 3,
        scratch_shapes=[
            pltpu.VMEM((rows_all, width), BF16),
            pltpu.VMEM((width, rows_all), BF16),
            pltpu.VMEM((rows_all, vocab), F32),
            pltpu.VMEM((rows_all, width), F32),
            pltpu.VMEM((2, rows_all, CHUNK), BF16),
            cell(F32), cell(F32), cell(F32), cell(F32), cell(F32), cell(F32), cell(jnp.int32),
            diag, diag, diag, diag, diag, diag,
            pltpu.VMEM((SLOT * utts, pred_dim), BF16),
            pltpu.VMEM((SLOT * utts, width), F32),
            pltpu.VMEM((utts, frames, width), BF16),
            pltpu.VMEM((8, vocab), F32),
            pltpu.VMEM((2, width // LANES, width, LANES), F32),
            pltpu.VMEM((2, side_rows - width // LANES * width, LANES), F32),
            pltpu.VMEM((width, vocab), BF16),
            pltpu.SemaphoreType.DMA((2,)),
            pltpu.SemaphoreType.DMA((2, width // LANES + 1)),
            pltpu.SemaphoreType.DMA(()),
            pltpu.SemaphoreType.DMA(()),
        ],
        compiler_params=pltpu.CompilerParams(vmem_limit_bytes=66_000_000),
        name="local_grads",
    )(labels, frame_len, label_len, enc, pred, w_enc, w_pred, b_joint.reshape(1, width), w_out, b_out.reshape(1, vocab))


def exchange_kernel(
    chunks, side_ref, dlog_ref, hid_t_ref, full, squares_ref, held, from_core, arrived, d_buf,
    side_sems, d_sems, core_sems, step_sems, extra_sems,
):
    dp, x = lax.axis_index("dp"), lax.axis_index("rep")
    core = lax.rem(dp, 2)
    place = (x, dp // 8, lax.rem(dp // 2, 4))
    width = hid_t_ref.shape[0]
    extra_at = chunks * PER_CHUNK

    def device(x, y, z, core):
        return ((y * 4 + z) * 2 + core, x)

    other_core = device(*place, 1 - core)

    def link(turn, s):
        axis = (turn + s) % 3
        v = place[axis]
        second = lax.rem((turn + s) // 3 + core, 2)
        peer = second * (3 - v) + (1 - second) * (v + 1 - 2 * lax.rem(v, 2))
        bit = second * (v // 2) + (1 - second) * lax.rem((v + 1) // 2, 2)
        where = list(place)
        where[axis] = peer
        return device(*where, core), bit

    barrier = pltpu.get_barrier_semaphore()
    peers = [other_core] + [link(p, 0)[0] for p in range(6)]
    for peer in peers:
        pl.semaphore_signal(barrier, inc=1, device_id=peer, device_id_type=pl.DeviceIdType.MESH)

    side_copies = []
    for h in range(2):
        for n, (src, dst, units) in enumerate(((0, 0, PER_CHUNK), (PER_CHUNK, extra_at, EXTRA))):
            copy = pltpu.make_async_copy(
                side_ref.at[h, pl.ds(src, units)], held.at[h, pl.ds(dst, units)], side_sems.at[h, n]
            )
            copy.start()
            side_copies.append(copy)

    def load_block(c):
        slot = lax.rem(c, 2)
        cols = pl.ds(pl.multiple_of((c - 1) * BLOCK, BLOCK), BLOCK)
        return pltpu.make_async_copy(dlog_ref.at[:, cols], d_buf.at[slot], d_sems.at[slot])

    load_block(1).start()

    turns = list(range(PER_CHUNK)) + [5, 2]
    offsets = []
    for turn in turns:
        line = [0]
        for s in range(6):
            line.append(line[-1] + link(turn, s)[1] * (UNIT >> (s + 1)))
        offsets.append(line)

    def rows(start, n):
        return pl.ds(pl.multiple_of(start, 8), n)

    def remote(src, dst, sems, index, peer):
        return pltpu.make_async_remote_copy(
            src_ref=src, dst_ref=dst, send_sem=sems.at[(*index, 0)], recv_sem=sems.at[(*index, 1)],
            device_id=peer, device_id_type=pl.DeviceIdType.MESH,
        )

    def unit_of(c, j):
        return c * PER_CHUNK + j if j < PER_CHUNK else extra_at + j - PER_CHUNK

    def sem_of(c, j, n):
        return (step_sems, (c, j, n)) if j < PER_CHUNK else (extra_sems, (j - PER_CHUNK, n))

    def swap(c, extra):
        units = pl.ds(extra_at, EXTRA) if extra else pl.ds(c * PER_CHUNK, PER_CHUNK)
        return remote(
            held.at[1 - core, units], from_core.at[units], core_sems, (chunks if extra else c,), other_core
        )

    def reduce(c, j, s):
        peer, bit = link(turns[j], s)
        n = UNIT >> (s + 1)
        u = unit_of(c, j)
        return remote(
            held.at[core, u, rows(offsets[j][s] + (1 - bit) * n, n)],
            arrived.at[u, pl.ds(UNIT - 2 * n, n)],
            *sem_of(c, j, s), peer,
        )

    def add_reduce(c, j, s):
        n = UNIT >> (s + 1)
        u = unit_of(c, j)
        here = rows(offsets[j][s + 1], n)
        total = held[core, u, here, :] + arrived[u, pl.ds(UNIT - 2 * n, n), :]
        if s < 5:
            held[core, u, here, :] = total
        else:
            full[core, u, here, :] = total

    def gather(c, j, s):
        here = full.at[core, unit_of(c, j), rows(offsets[j][s + 1], UNIT >> (s + 1))]
        return remote(here, here, *sem_of(c, j, 6 + s), link(turns[j], s)[0])

    def give(c, j, late):
        n = UNIT // 2
        bit = link(turns[j], 0)[1]
        start = (1 - bit) * n if late else bit * n
        here = full.at[core, unit_of(c, j), rows(start, n)]
        return remote(here, here, *sem_of(c, j, 13 if late else 12), other_core)

    def stage(k, c, lanes):
        if k == 1:
            for extra in {j >= PER_CHUNK for j in lanes}:
                swap(c, extra).wait()
                units = pl.ds(extra_at, EXTRA) if extra else pl.ds(c * PER_CHUNK, PER_CHUNK)
                held[core, units] = held[core, units] + from_core[units]
            for j in lanes:
                reduce(c, j, 0).start()
        elif k <= 7:
            for j in lanes:
                reduce(c, j, k - 2).wait()
                add_reduce(c, j, k - 2)
            for j in lanes:
                if k < 7:
                    reduce(c, j, k - 1).start()
                else:
                    gather(c, j, 5).start()
        elif k <= 12:
            for j in lanes:
                gather(c, j, 13 - k).wait()
                gather(c, j, 12 - k).start()
                if k == 12:
                    give(c, j, False).start()
        elif k == 13:
            for j in lanes:
                gather(c, j, 0).wait()
                give(c, j, True).start()
        else:
            for j in lanes:
                give(c, j, False).wait()
                give(c, j, True).wait()

    stages = 14
    pl.semaphore_wait(barrier, len(peers))

    def tick(t, carry):
        for k in range(stages, 0, -1):

            @pl.when((t >= GAP * k) & (t < chunks + GAP * k))
            def _(k=k):
                stage(k, t - GAP * k, range(PER_CHUNK))

            @pl.when(t == GAP * k)
            def _(k=k):
                stage(k, 0, range(PER_CHUNK, PER_CHUNK + EXTRA))

        @pl.when(t == 0)
        def _():
            for copy in side_copies:
                copy.wait()
            swap(0, False).start()
            swap(0, True).start()

        @pl.when((t >= 1) & (t < chunks))
        def _():
            load_block(t).wait()

            @pl.when(t + 1 < chunks)
            def _():
                load_block(t + 1).start()

            slot = lax.rem(t, 2)
            for h in range(2):
                g = jnp.dot(
                    hid_t_ref[...], d_buf[slot, :, h * BLOCK // 2 : (h + 1) * BLOCK // 2], preferred_element_type=F32
                )
                tiles = jnp.concatenate([g[:, k * LANES : (k + 1) * LANES] for k in range(4)], axis=0)
                held[h, pl.ds(t * PER_CHUNK, PER_CHUNK)] = tiles.reshape(PER_CHUNK, UNIT, LANES)
            swap(t, False).start()

        return carry

    lax.fori_loop(0, chunks + GAP * stages, tick, 0)

    block, lines = 1024, 64
    total = jnp.zeros((lines, LANES), F32)
    for h in range(2):

        def add_squares(u, total, h=h):
            here = full[h, u].reshape(UNIT // lines, lines, LANES)
            return total + jnp.sum(here * here, axis=0)

        total = lax.fori_loop(0, extra_at + 1, add_squares, total)
        left = width - UNIT if h else EXTRA * UNIT - UNIT
        here = full[h, extra_at + 1, 0:left, :].reshape(left // lines, lines, LANES)
        total = total + jnp.sum(here * here, axis=0)
    squares_ref[...] = jnp.sum(total.reshape(lines // 8, 8, LANES), axis=0)


def exchange(side, dlog, hid_t):
    width, rows_all = hid_t.shape
    vocab = dlog.shape[1]
    chunks, main, half = layout(width, vocab)
    units = half // UNIT
    vmem = pl.BlockSpec(memory_space=pltpu.VMEM)
    anywhere = pl.BlockSpec(memory_space=pl.ANY)
    shape = jax.ShapeDtypeStruct
    full, squares = pl.pallas_call(
        functools.partial(exchange_kernel, chunks),
        out_shape=(shape((2, units, UNIT, LANES), F32), shape((8, LANES), F32)),
        in_specs=[anywhere, anywhere, vmem],
        out_specs=(vmem, vmem),
        scratch_shapes=[
            pltpu.VMEM((2, units, UNIT, LANES), F32),
            pltpu.VMEM((units, UNIT, LANES), F32),
            pltpu.VMEM((units, UNIT, LANES), F32),
            pltpu.VMEM((2, rows_all, BLOCK), BF16),
            pltpu.SemaphoreType.DMA((2, 2)),
            pltpu.SemaphoreType.DMA((2,)),
            pltpu.SemaphoreType.DMA((chunks + 1, 2)),
            pltpu.SemaphoreType.DMA((chunks, PER_CHUNK, 14, 2)),
            pltpu.SemaphoreType.DMA((EXTRA, 14, 2)),
        ],
        compiler_params=pltpu.CompilerParams(collective_id=0, has_side_effects=True, vmem_limit_bytes=63_000_000),
        name="exchange",
    )(side.reshape(2, side.shape[1] // UNIT, UNIT, LANES), dlog, hid_t)
    return full.reshape(2 * half, LANES), squares


def finish_kernel(main, half, count, full, squares_ref, out_ref, enc_ref, pred_ref, bias_ref, joint_ref, loss_ref, buf, side_buf, sems):
    width, vocab = out_ref.shape
    squares = jnp.sum(jnp.sum(squares_ref[...], axis=0, keepdims=True), axis=1, keepdims=True)
    scale = lax.rsqrt(squares * (1.0 / count) + EPS)
    copies = []
    steps = vocab // CHUNK
    per = CHUNK // LANES
    for c in range(steps):
        slot = c % buf.shape[0]
        if c >= buf.shape[0]:
            copies[c - buf.shape[0]].wait()
        for k in range(per):
            v = c * per + k
            row = v % 8 // 4 * half + (v // 8 + 1) * main + v % 4 * width
            buf[slot, :, k * LANES : (k + 1) * LANES] = full[row : row + width, :] * scale
        copy = pltpu.make_async_copy(buf.at[slot], out_ref.at[:, pl.ds(c * CHUNK, CHUNK)], sems.at[slot])
        copy.start()
        copies.append(copy)
    extra = half - EXTRA * UNIT
    side_copies = []
    for i, ref in enumerate((enc_ref, pred_ref)):
        for k in range(width // LANES):
            row = i * half + (k * width if k < 4 else extra)
            side_buf[i, :, k * LANES : (k + 1) * LANES] = full[row : row + width, :] * scale
        copy = pltpu.make_async_copy(side_buf.at[i], ref, sems.at[buf.shape[0] + i])
        copy.start()
        side_copies.append(copy)
    row = extra + width
    for k in range(vocab // LANES):
        bias_ref[:, k * LANES : (k + 1) * LANES] = full[row + k : row + k + 1, :] * scale
    row += vocab // LANES
    for k in range(width // LANES):
        joint_ref[:, k * LANES : (k + 1) * LANES] = full[row + k : row + k + 1, :] * scale
    row = half + extra + width
    loss = jnp.sum(full[row : row + 1, :], axis=1, keepdims=True)
    labels = jnp.sum(full[row + 1 : row + 2, :], axis=1, keepdims=True)
    loss_ref[...] = jnp.broadcast_to(loss / labels, loss_ref.shape)
    for copy in copies[-buf.shape[0] :] + side_copies:
        copy.wait()


def finish(full, squares, width, vocab, count):
    _, main, half = layout(width, vocab)
    vmem = pl.BlockSpec(memory_space=pltpu.VMEM)
    anywhere = pl.BlockSpec(memory_space=pl.ANY)
    shape = jax.ShapeDtypeStruct
    return pl.pallas_call(
        functools.partial(finish_kernel, main, half, float(count)),
        out_shape=(
            shape((width, vocab), F32), shape((width, width), F32), shape((width, width), F32),
            shape((1, vocab), F32), shape((1, width), F32), shape((1, LANES), F32),
        ),
        in_specs=[vmem, vmem],
        out_specs=(anywhere, anywhere, anywhere, vmem, vmem, vmem),
        scratch_shapes=[
            pltpu.VMEM((4, width, CHUNK), F32),
            pltpu.VMEM((2, width, width), F32),
            pltpu.SemaphoreType.DMA((6,)),
        ],
        compiler_params=pltpu.CompilerParams(vmem_limit_bytes=40_000_000),
        name="finish",
    )(full, squares)


def per_device(enc, pred, labels, frame_len, label_len, w_enc, w_pred, b_joint, w_out, b_out):
    width, vocab = w_out.shape
    sums = local_grads(enc, pred, labels, frame_len, label_len, w_enc, w_pred, b_joint, w_out, b_out)
    full, squares = exchange(*sums)
    count = w_enc.size + w_pred.size + w_out.size + b_out.size + b_joint.size
    out, g_enc, g_pred, bias, joint, loss = finish(full, squares, width, vocab, count)
    return g_enc, g_pred, out, bias.reshape(vocab), joint.reshape(width), loss[0, 0]


def solution(mesh):
    split = P(AXES)
    in_specs = (split, split, split, split, split, P(), P(), P(), P(), P())
    return jax.shard_map(per_device, mesh=mesh, in_specs=in_specs, out_specs=(P(),) * 6, check_vma=False)
```

```python
import functools

import jax
import jax.numpy as jnp
from jax import lax
from jax.experimental import pallas as pl
from jax.experimental.pallas import tpu as pltpu
from jax.sharding import PartitionSpec as P

AXES = ("dp", "rep")
NEG = -1e30
EPS = 1e-06
F32 = jnp.float32
BF16 = jnp.bfloat16
LANES = 128
SLOT = 32
CHUNK = 512
ROWS = 416


def local_kernel(
    labels_ref, frame_ref, label_ref, enc_ref, pred_ref, w_enc_ref, w_pred_ref, b_joint_ref, w_out_hbm, b_out_ref,
    side_ref, dlog_ref, hid_t_ref,
    hid, hid_t, logits, dhid, dlog, top, tot, lse, occ, emit_occ, blank_occ, target, blank_d, emit_d, alpha_d,
    beta_d, below_d, right_d, pred_pad, dpred_pad, denc, bias_acc, slabs, tail, w_out_ref, sems, side_sems, load_sem, hid_sem,
):
    utts, frames, _ = enc_ref.shape
    slots = pred_ref.shape[1]
    width = w_enc_ref.shape[1]
    vocab = w_out_ref.shape[1]
    rows_all = hid.shape[0]
    load = pltpu.make_async_copy(w_out_hbm, w_out_ref, load_sem)
    load.start()
    cells = utts * slots * frames
    diags = frames + slots - 1
    blocks = [(i, u, (i * slots + u) * frames, SLOT * i + u) for i in range(utts) for u in range(slots)]
    lane_row = lax.broadcasted_iota(jnp.int32, (1, LANES), 1)
    lane_cell = lax.broadcasted_iota(jnp.int32, (frames, LANES), 1)

    def label_at(i, u):
        return labels_ref[i, u] if u < slots - 1 else 1

    pred_pad[...] = jnp.zeros_like(pred_pad)
    hid[cells:, :] = jnp.zeros((rows_all - cells, width), BF16)
    enc_proj = [jnp.dot(enc_ref[i], w_enc_ref[...], preferred_element_type=F32) for i in range(utts)]
    for i in range(utts):
        pred_pad[SLOT * i : SLOT * i + slots, :] = pred_ref[i]
    pred_proj = jnp.dot(pred_pad[...], w_pred_ref[...], preferred_element_type=F32) + b_joint_ref[...].astype(F32)
    for i, u, row, col in blocks:
        hid[row : row + frames, :] = jnp.tanh(enc_proj[i] + pred_proj[col : col + 1, :]).astype(BF16)
    hid_t[...] = hid[...].T
    hid_copy = pltpu.make_async_copy(hid_t, hid_t_ref, hid_sem)
    hid_copy.start()
    load.wait()

    label_row = jnp.full((1, LANES), -1, jnp.int32)
    for i, u, row, col in blocks:
        label_row = jnp.where(lane_row == col, label_at(i, u), label_row)
    picks = lax.broadcasted_iota(jnp.int32, (vocab, LANES), 0) == label_row
    picks = picks.astype(F32).astype(BF16)
    w_pick = jnp.dot(w_out_ref[...], picks, preferred_element_type=F32).astype(BF16)
    b_pick = jnp.dot(
        jnp.broadcast_to(b_out_ref[...], (16, vocab)), picks, preferred_element_type=F32
    )[:1, :]
    w_blank = jnp.broadcast_to(w_out_ref[:, :1].astype(F32), (width, LANES)).astype(BF16)
    w_two = jnp.concatenate([w_pick, w_blank], axis=1)
    b_blank = b_out_ref[:, :1].astype(F32)

    top[...] = jnp.full_like(top, NEG)
    tot[...] = jnp.zeros_like(tot)

    def forward(c, carry):
        cols = pl.ds(pl.multiple_of(c * CHUNK, CHUNK), CHUNK)
        w_c = w_out_ref[:, cols]
        b_c = b_out_ref[:, cols].astype(F32)
        for r in range(0, rows_all, ROWS):
            z = jnp.dot(hid[r : r + ROWS, :], w_c, preferred_element_type=F32) + b_c
            logits[r : r + ROWS, cols] = z
            tiles = [z[:, k : k + LANES] for k in range(0, CHUNK, LANES)]
            old = top[r : r + ROWS, :]
            new = functools.reduce(jnp.maximum, tiles, old)
            top[r : r + ROWS, :] = new
            tot[r : r + ROWS, :] = tot[r : r + ROWS, :] * jnp.exp(old - new) + sum(jnp.exp(t - new) for t in tiles)
        return carry

    lax.fori_loop(0, vocab // CHUNK, forward, 0)

    for r in range(0, rows_all, ROWS):
        row_top = jnp.max(top[r : r + ROWS, :], axis=1, keepdims=True)
        row_sum = jnp.sum(tot[r : r + ROWS, :] * jnp.exp(top[r : r + ROWS, :] - row_top), axis=1, keepdims=True)
        row_lse = jnp.broadcast_to(row_top + jnp.log(row_sum), (ROWS, LANES))
        lse[r : r + ROWS, :] = row_lse
        two = jnp.dot(hid[r : r + ROWS, :], w_two, preferred_element_type=F32)
        top[r : r + ROWS, :] = two[:, :LANES] + b_pick - row_lse
        tot[r : r + ROWS, :] = two[:, LANES:] + b_blank - row_lse

    blank_d[...] = jnp.full_like(blank_d, NEG)
    emit_d[...] = jnp.full_like(emit_d, NEG)
    for i, u, row, col in blocks:
        here = lane_cell == col
        emit_d[u : u + frames, :] = jnp.where(here, top[row : row + frames, :], emit_d[u : u + frames, :])
        blank_d[u : u + frames, :] = jnp.where(here, tot[row : row + frames, :], blank_d[u : u + frames, :])
    label_pos = lax.rem(lane_row, SLOT)
    frame_count = jnp.full((1, LANES), 0, jnp.int32)
    label_count = jnp.full((1, LANES), -1, jnp.int32)
    for i in range(utts):
        mine = lane_row // SLOT == i
        frame_count = jnp.where(mine, frame_ref[i], frame_count)
        label_count = jnp.where(mine, label_ref[i], label_count)

    def join(a, b):
        hi = jnp.maximum(a, b)
        return hi + jnp.log(1.0 + jnp.exp(jnp.minimum(a, b) - hi))

    alpha = jnp.where((label_pos == 0) & (lane_row < SLOT * utts), 0.0, NEG).astype(F32)
    beta = jnp.full((1, LANES), NEG, F32)
    alpha_d[0:1, :] = alpha
    for step in range(diags):
        d = diags - 1 - step
        t = d - label_pos
        live = (t >= 0) & (t < frame_count) & (label_pos <= label_count)
        last = (t == frame_count - 1) & (label_pos == label_count)
        below = jnp.where(last, 0.0, beta)
        right = pltpu.roll(beta, LANES - 1, 1)
        below_d[d : d + 1, :] = below
        right_d[d : d + 1, :] = right
        beta = jnp.where(live, join(below + blank_d[d : d + 1, :], right + emit_d[d : d + 1, :]), NEG)
        beta_d[d : d + 1, :] = beta
        if step > 0:
            left = pltpu.roll(alpha + emit_d[step - 1 : step, :], 1, 1)
            alpha = join(alpha + blank_d[step - 1 : step, :], left)
            alpha_d[step : step + 1, :] = alpha
    total = jnp.full((1, LANES), 0.0, F32)
    for i in range(utts):
        beta_0 = jnp.sum(jnp.where(lane_row == SLOT * i, beta, 0.0), axis=1, keepdims=True)
        total = jnp.where(lane_row // SLOT == i, beta_0, total)
    span = slice(0, diags)
    blank_d[span, :] = jnp.exp(
        jnp.minimum(alpha_d[span, :] + blank_d[span, :] + below_d[span, :] - total, 80.0)
    )
    emit_d[span, :] = jnp.exp(jnp.minimum(alpha_d[span, :] + emit_d[span, :] + right_d[span, :] - total, 80.0))

    pad = slice(cells, rows_all)
    occ[pad, :] = jnp.zeros((rows_all - cells, LANES), F32)
    emit_occ[pad, :] = jnp.zeros((rows_all - cells, LANES), F32)
    blank_occ[pad, :] = jnp.zeros((rows_all - cells, LANES), F32)
    target[pad, :] = jnp.full((rows_all - cells, LANES), -1, jnp.int32)
    for i, u, row, col in blocks:
        here = slice(row, row + frames)
        b = jnp.broadcast_to(blank_d[u : u + frames, col : col + 1], (frames, LANES))
        e = jnp.broadcast_to(emit_d[u : u + frames, col : col + 1], (frames, LANES))
        blank_occ[here, :] = b
        emit_occ[here, :] = e
        occ[here, :] = b + e
        target[here, :] = jnp.full((frames, LANES), label_at(i, u), jnp.int32)

    dhid[...] = jnp.zeros_like(dhid)

    bias_acc[...] = jnp.zeros_like(bias_acc)

    def out_copy(c, slot):
        cols = pl.ds(pl.multiple_of(c * CHUNK, CHUNK), CHUNK)
        return pltpu.make_async_copy(dlog.at[slot], dlog_ref.at[:, cols], sems.at[slot])

    def backward(c, carry):
        cols = pl.ds(pl.multiple_of(c * CHUNK, CHUNK), CHUNK)
        slot = lax.rem(c, 2)
        w_c = w_out_ref[:, cols]
        first = c == 0

        @pl.when(c >= 2)
        def _():
            out_copy(c - 2, slot).wait()

        sums = [jnp.zeros((8, LANES), F32)] * (CHUNK // LANES)
        for r in range(0, rows_all, ROWS):
            here = slice(r, r + ROWS)
            row_lse, row_occ, row_emit = lse[here, :], occ[here, :], emit_occ[here, :]
            row_target = target[here, :] - c * CHUNK
            lane = lax.broadcasted_iota(jnp.int32, (ROWS, LANES), 1)
            parts = []
            for k in range(0, CHUNK, LANES):
                z = logits[here, pl.ds(pl.multiple_of(c * CHUNK + k, LANES), LANES)]
                d = jnp.exp(z - row_lse) * row_occ - jnp.where(lane + k == row_target, row_emit, 0.0)
                if k == 0:
                    d = d - jnp.where((lane == 0) & first, blank_occ[here, :], 0.0)
                sums[k // LANES] = sums[k // LANES] + jnp.sum(d.reshape(ROWS // 8, 8, LANES), axis=0)
                parts.append(d.astype(BF16))
            d = jnp.concatenate(parts, axis=1)
            dlog[slot, here, :] = d
            dhid[here, :] += lax.dot_general(d, w_c, (((1,), (1,)), ((), ())), preferred_element_type=F32)
        bias_acc[:, cols] = jnp.concatenate(sums, axis=1)
        out_copy(c, slot).start()
        return carry

    steps = vocab // CHUNK
    lax.fori_loop(0, steps, backward, 0)

    dpred_pad[...] = jnp.zeros_like(dpred_pad)
    for i in range(utts):
        enc_sum = jnp.zeros((frames, width), F32)
        for u in range(slots):
            row = (i * slots + u) * frames
            h = hid[row : row + frames, :].astype(F32)
            dpre = dhid[row : row + frames, :] * (1.0 - h * h)
            enc_sum = enc_sum + dpre
            dpred_pad[SLOT * i + u : SLOT * i + u + 1, :] = jnp.sum(dpre, axis=0, keepdims=True)
        denc[i] = enc_sum.astype(BF16)
    dpred = dpred_pad[...].astype(BF16)
    over_rows = (((0,), (0,)), ((), ()))
    g_enc = jnp.zeros((width, width), F32)
    for i in range(utts):
        g_enc = g_enc + lax.dot_general(enc_ref[i], denc[i], over_rows, preferred_element_type=F32)
    g_pred = lax.dot_general(pred_pad[...], dpred, over_rows, preferred_element_type=F32)
    per = width // LANES
    last_copies = []
    for i, g in enumerate((g_enc, g_pred)):
        for k in range(per):
            slabs[i, k] = g[:, k * LANES : (k + 1) * LANES]
        for k in range(per):
            last_copies.append(
                pltpu.make_async_copy(slabs.at[i, k], side_ref.at[i, pl.ds(k * width, width), :], side_sems.at[i, k])
            )
            last_copies[-1].start()
    tail[...] = jnp.zeros_like(tail)
    bias = jnp.sum(bias_acc[...], axis=0, keepdims=True)
    joint = jnp.sum(dpred.astype(F32), axis=0, keepdims=True)
    for k in range(vocab // LANES):
        tail[0, k : k + 1, :] = bias[:, k * LANES : (k + 1) * LANES]
    for k in range(per):
        tail[0, vocab // LANES + k : vocab // LANES + k + 1, :] = joint[:, k * LANES : (k + 1) * LANES]
    head = (lax.rem(lane_row, SLOT) == 0) & (lane_row < SLOT * utts)
    tail[1, 0:1, :] = jnp.where(head, -beta_d[0:1, :], 0.0)
    tail[1, 1:2, :] = jnp.where(head, label_count.astype(F32), 0.0)
    for i in range(2):
        last_copies.append(
            pltpu.make_async_copy(
                tail.at[i], side_ref.at[i, pl.ds(per * width, tail.shape[1]), :], side_sems.at[i, per]
            )
        )
        last_copies[-1].start()
    for c in range(max(0, steps - 2), steps):
        out_copy(c, c % 2).wait()
    hid_copy.wait()
    for copy in last_copies:
        copy.wait()


UNIT = 512
PER_CHUNK = 5
BLOCK = 1024
GAP = 2
GROUPS = ((0,), (1,), (2, 3), (4, 5))
EXTRA = 2


def layout(width, vocab):
    chunks = 1 + vocab // BLOCK
    main = PER_CHUNK * UNIT
    half = chunks * main + EXTRA * UNIT
    per = width // LANES
    assert main == 4 * width and BLOCK == 8 * LANES and per == 5
    return chunks, main, half


def local_grads(enc, pred, labels, frame_len, label_len, w_enc, w_pred, b_joint, w_out, b_out):
    utts, frames, enc_dim = enc.shape
    slots, pred_dim = pred.shape[1:]
    width, vocab = w_out.shape
    rows_all = -(-utts * slots * frames // ROWS) * ROWS
    diags = frames + slots
    diag_rows = -(-diags // 8) * 8
    chunks, main, half = layout(width, vocab)
    side_rows = main + EXTRA * UNIT
    shape = jax.ShapeDtypeStruct
    smem = pl.BlockSpec(memory_space=pltpu.SMEM)
    vmem = pl.BlockSpec(memory_space=pltpu.VMEM)
    anywhere = pl.BlockSpec(memory_space=pl.ANY)
    cell = lambda t: pltpu.VMEM((rows_all, LANES), t)
    diag = pltpu.VMEM((diag_rows, LANES), F32)
    return pl.pallas_call(
        local_kernel,
        out_shape=(
            shape((2, side_rows, LANES), F32), shape((rows_all, vocab), BF16), shape((width, rows_all), BF16),
        ),
        in_specs=[smem] * 3 + [vmem] * 5 + [anywhere, vmem],
        out_specs=(anywhere,) * 3,
        scratch_shapes=[
            pltpu.VMEM((rows_all, width), BF16),
            pltpu.VMEM((width, rows_all), BF16),
            pltpu.VMEM((rows_all, vocab), F32),
            pltpu.VMEM((rows_all, width), F32),
            pltpu.VMEM((2, rows_all, CHUNK), BF16),
            cell(F32), cell(F32), cell(F32), cell(F32), cell(F32), cell(F32), cell(jnp.int32),
            diag, diag, diag, diag, diag, diag,
            pltpu.VMEM((SLOT * utts, pred_dim), BF16),
            pltpu.VMEM((SLOT * utts, width), F32),
            pltpu.VMEM((utts, frames, width), BF16),
            pltpu.VMEM((8, vocab), F32),
            pltpu.VMEM((2, width // LANES, width, LANES), F32),
            pltpu.VMEM((2, side_rows - width // LANES * width, LANES), F32),
            pltpu.VMEM((width, vocab), BF16),
            pltpu.SemaphoreType.DMA((2,)),
            pltpu.SemaphoreType.DMA((2, width // LANES + 1)),
            pltpu.SemaphoreType.DMA(()),
            pltpu.SemaphoreType.DMA(()),
        ],
        compiler_params=pltpu.CompilerParams(vmem_limit_bytes=66_000_000),
        name="local_grads",
    )(labels, frame_len, label_len, enc, pred, w_enc, w_pred, b_joint.reshape(1, width), w_out, b_out.reshape(1, vocab))


def exchange_kernel(
    chunks, side_ref, dlog_ref, hid_t_ref, full_ref, squares_ref, full, held, from_core, arrived, d_buf, total_ref,
    out_sems, side_sems, d_sems, core_sems, step_sems, extra_sems,
):
    dp, x = lax.axis_index("dp"), lax.axis_index("rep")
    core = lax.rem(dp, 2)
    place = (x, dp // 8, lax.rem(dp // 2, 4))
    width = hid_t_ref.shape[0]
    extra_at = chunks * PER_CHUNK

    def device(x, y, z, core):
        return ((y * 4 + z) * 2 + core, x)

    other_core = device(*place, 1 - core)

    def link(turn, s):
        axis = (turn + s) % 3
        v = place[axis]
        second = lax.rem((turn + s) // 3 + core, 2)
        peer = second * (3 - v) + (1 - second) * (v + 1 - 2 * lax.rem(v, 2))
        bit = second * (v // 2) + (1 - second) * lax.rem((v + 1) // 2, 2)
        return axis, peer, bit

    def peers_of(turn, group):
        found = []
        for mask in range(1, 1 << len(group)):
            flips = [i for i in range(len(group)) if mask >> i & 1]
            where = list(place)
            for i in flips:
                axis, peer, _ = link(turn, group[i])
                where[axis] = peer
            found.append((flips, device(*where, core)))
        return found

    turns = list(range(PER_CHUNK)) + [5, 2]
    bits = [[link(turn, s)[2] for s in range(6)] for turn in turns]
    barrier = pltpu.get_barrier_semaphore()
    greeted = {}
    for turn in range(6):
        for group in GROUPS:
            for flips, peer in peers_of(turn, group):
                key = frozenset((turn + group[i]) % 6 for i in flips)
                greeted[key] = peer
    peers = [other_core] + list(greeted.values())
    for peer in peers:
        pl.semaphore_signal(barrier, inc=1, device_id=peer, device_id_type=pl.DeviceIdType.MESH)

    side_copies = []
    for h in range(2):
        for n, (src, dst, units) in enumerate(((0, 0, PER_CHUNK), (PER_CHUNK, extra_at, EXTRA))):
            copy = pltpu.make_async_copy(
                side_ref.at[h, pl.ds(src, units)], held.at[h, pl.ds(dst, units)], side_sems.at[h, n]
            )
            copy.start()
            side_copies.append(copy)

    def load_block(c):
        slot = lax.rem(c, 2)
        cols = pl.ds(pl.multiple_of((c - 1) * BLOCK, BLOCK), BLOCK)
        return pltpu.make_async_copy(dlog_ref.at[:, cols], d_buf.at[slot], d_sems.at[slot])

    load_block(1).start()

    offsets = []
    for line_bits in bits:
        line = [0]
        for s in range(6):
            line.append(line[-1] + line_bits[s] * (UNIT >> (s + 1)))
        offsets.append(line)

    def rows(start, n):
        return pl.ds(pl.multiple_of(start, 8), n)

    def remote(src, dst, sems, index, peer):
        return pltpu.make_async_remote_copy(
            src_ref=src, dst_ref=dst, send_sem=sems.at[(*index, 0)], recv_sem=sems.at[(*index, 1)],
            device_id=peer, device_id_type=pl.DeviceIdType.MESH,
        )

    def unit_of(c, j):
        return c * PER_CHUNK + j if j < PER_CHUNK else extra_at + j - PER_CHUNK

    def sem_of(c, j, n):
        return (step_sems, (c, j, n)) if j < PER_CHUNK else (extra_sems, (j - PER_CHUNK, n))

    def swap(c, extra):
        units = pl.ds(extra_at, EXTRA) if extra else pl.ds(c * PER_CHUNK, PER_CHUNK)
        return remote(
            held.at[1 - core, units], from_core.at[units], core_sems, (chunks if extra else c,), other_core
        )

    lands, numbers = [], []
    at = number = 0
    for group in GROUPS:
        count = (1 << len(group)) - 1
        lands.append(at)
        numbers.append(number)
        at += count * (UNIT >> (group[-1] + 1))
        number += count
    per_way = number

    def reduce(c, j, g):
        group = GROUPS[g]
        n = UNIT >> (group[-1] + 1)
        u = unit_of(c, j)
        copies = []
        for m, (flips, peer) in enumerate(peers_of(turns[j], group)):
            start = offsets[j][group[0]]
            for i, s in enumerate(group):
                bit = bits[j][s]
                start = start + (1 - bit if i in flips else bit) * (UNIT >> (s + 1))
            copies.append(
                remote(
                    held.at[core, u, rows(start, n)], arrived.at[u, pl.ds(lands[g] + m * n, n)],
                    *sem_of(c, j, numbers[g] + m), peer,
                )
            )
        return copies

    def add_reduce(c, j, g):
        group = GROUPS[g]
        n = UNIT >> (group[-1] + 1)
        u = unit_of(c, j)
        here = rows(offsets[j][group[-1] + 1], n)
        total = held[core, u, here, :]
        for m in range((1 << len(group)) - 1):
            total = total + arrived[u, pl.ds(lands[g] + m * n, n), :]
        if g < len(GROUPS) - 1:
            held[core, u, here, :] = total
        else:
            full[core, u, here, :] = total

    def gather(c, j, g):
        group = GROUPS[g]
        here = full.at[core, unit_of(c, j), rows(offsets[j][group[-1] + 1], UNIT >> (group[-1] + 1))]
        return [
            remote(here, here, *sem_of(c, j, per_way + numbers[g] + m), peer)
            for m, (_, peer) in enumerate(peers_of(turns[j], group))
        ]

    def give(c, j, late):
        n = UNIT // 2
        bit = bits[j][0]
        start = (1 - bit) * n if late else bit * n
        here = full.at[core, unit_of(c, j), rows(start, n)]
        return [remote(here, here, *sem_of(c, j, 2 * per_way + late), other_core)]

    def put(c, extra):
        units = pl.ds(extra_at, EXTRA) if extra else pl.ds(c * PER_CHUNK, PER_CHUNK)
        return [
            pltpu.make_async_copy(full.at[h, units], full_ref.at[h, units], out_sems.at[chunks if extra else c, h])
            for h in range(2)
        ]

    def start(copies):
        for copy in copies:
            copy.start()

    def wait(copies):
        for copy in copies:
            copy.wait()

    lines = 64

    def add_squares(here):
        here = here.reshape(here.shape[0] // lines, lines, LANES)
        total_ref[...] = total_ref[...] + jnp.sum(here * here, axis=0)

    last = len(GROUPS) - 1

    def stage(k, c, lanes):
        extra = lanes[0] >= PER_CHUNK
        if k == 1:
            swap(c, extra).wait()
            units = pl.ds(extra_at, EXTRA) if extra else pl.ds(c * PER_CHUNK, PER_CHUNK)
            held[core, units] = held[core, units] + from_core[units]
            for j in lanes:
                start(reduce(c, j, 0))
        elif k <= last + 2:
            for j in lanes:
                wait(reduce(c, j, k - 2))
                add_reduce(c, j, k - 2)
            for j in lanes:
                start(reduce(c, j, k - 1) if k <= last + 1 else gather(c, j, last))
        elif k <= 2 * last + 2:
            g = 2 * last + 2 - k
            for j in lanes:
                wait(gather(c, j, g + 1))
                start(gather(c, j, g))
                if g == 0:
                    start(give(c, j, 0))
        elif k == 2 * last + 3:
            for j in lanes:
                wait(gather(c, j, 0))
                start(give(c, j, 1))
        else:
            for j in lanes:
                wait(give(c, j, 0))
                wait(give(c, j, 1))
            start(put(c, extra))
            for h in range(2):
                if extra:
                    left = width - UNIT if h else EXTRA * UNIT - UNIT
                    add_squares(full[h, extra_at])
                    add_squares(full[h, extra_at + 1, 0:left, :])
                else:
                    for j in lanes:
                        add_squares(full[h, unit_of(c, j)])

    stages = 2 * last + 4
    total_ref[...] = jnp.zeros_like(total_ref)
    pl.semaphore_wait(barrier, len(peers))

    def tick(t, carry):
        for k in range(stages, 0, -1):

            @pl.when((t >= GAP * k) & (t < chunks + GAP * k))
            def _(k=k):
                stage(k, t - GAP * k, range(PER_CHUNK))

            @pl.when(t == GAP * k)
            def _(k=k):
                stage(k, 0, range(PER_CHUNK, PER_CHUNK + EXTRA))

        @pl.when(t == 0)
        def _():
            for copy in side_copies:
                copy.wait()
            swap(0, False).start()
            swap(0, True).start()

        @pl.when((t >= 1) & (t < chunks))
        def _():
            load_block(t).wait()

            @pl.when(t + 1 < chunks)
            def _():
                load_block(t + 1).start()

            slot = lax.rem(t, 2)
            for h in range(2):
                g = jnp.dot(
                    hid_t_ref[...], d_buf[slot, :, h * BLOCK // 2 : (h + 1) * BLOCK // 2], preferred_element_type=F32
                )
                tiles = jnp.concatenate([g[:, k * LANES : (k + 1) * LANES] for k in range(4)], axis=0)
                held[h, pl.ds(t * PER_CHUNK, PER_CHUNK)] = tiles.reshape(PER_CHUNK, UNIT, LANES)
            swap(t, False).start()

        return carry

    lax.fori_loop(0, chunks + GAP * stages, tick, 0)

    squares_ref[...] = jnp.sum(total_ref[...].reshape(lines // 8, 8, LANES), axis=0)
    for c in range(chunks):
        wait(put(c, False))
    wait(put(0, True))


def exchange(side, dlog, hid_t):
    width, rows_all = hid_t.shape
    vocab = dlog.shape[1]
    chunks, main, half = layout(width, vocab)
    units = half // UNIT
    messages = 2 * sum((1 << len(group)) - 1 for group in GROUPS) + 2
    vmem = pl.BlockSpec(memory_space=pltpu.VMEM)
    anywhere = pl.BlockSpec(memory_space=pl.ANY)
    shape = jax.ShapeDtypeStruct
    full, squares = pl.pallas_call(
        functools.partial(exchange_kernel, chunks),
        out_shape=(shape((2, units, UNIT, LANES), F32), shape((8, LANES), F32)),
        in_specs=[anywhere, anywhere, vmem],
        out_specs=(anywhere, vmem),
        scratch_shapes=[
            pltpu.VMEM((2, units, UNIT, LANES), F32),
            pltpu.VMEM((2, units, UNIT, LANES), F32),
            pltpu.VMEM((units, UNIT, LANES), F32),
            pltpu.VMEM((units, UNIT, LANES), F32),
            pltpu.VMEM((2, rows_all, BLOCK), BF16),
            pltpu.VMEM((64, LANES), F32),
            pltpu.SemaphoreType.DMA((chunks + 1, 2)),
            pltpu.SemaphoreType.DMA((2, 2)),
            pltpu.SemaphoreType.DMA((2,)),
            pltpu.SemaphoreType.DMA((chunks + 1, 2)),
            pltpu.SemaphoreType.DMA((chunks, PER_CHUNK, messages, 2)),
            pltpu.SemaphoreType.DMA((EXTRA, messages, 2)),
        ],
        compiler_params=pltpu.CompilerParams(collective_id=0, has_side_effects=True, vmem_limit_bytes=63_000_000),
        name="exchange",
    )(side.reshape(2, side.shape[1] // UNIT, UNIT, LANES), dlog, hid_t)
    return full.reshape(2 * half, LANES), squares


def finish_kernel(main, half, count, full_ref, squares_ref, out_ref, enc_ref, pred_ref, bias_ref, joint_ref, loss_ref, full, buf, side_buf, load_sems, sems):
    width, vocab = out_ref.shape
    chunks = 1 + vocab // BLOCK
    loads = []
    for h in range(2):
        spans = [(c * main, main) for c in range(chunks)] + [(chunks * main, half - chunks * main)]
        for c, (at, n) in enumerate(spans):
            here = pl.ds(h * half + at, n)
            loads.append(pltpu.make_async_copy(full_ref.at[here, :], full.at[here, :], load_sems.at[h, c]))
    arrivals = {}
    for c in [*range(1, chunks), 0, chunks]:
        arrivals[c] = [loads[c], loads[c + chunks + 1]]
        for copy in arrivals[c]:
            copy.start()
    squares = jnp.sum(jnp.sum(squares_ref[...], axis=0, keepdims=True), axis=1, keepdims=True)
    scale = lax.rsqrt(squares * (1.0 / count) + EPS)
    copies = []
    steps = vocab // CHUNK
    per = CHUNK // LANES
    for c in range(steps):
        slot = c % buf.shape[0]
        if c >= buf.shape[0]:
            copies[c - buf.shape[0]].wait()
        arrivals[c // 2 + 1][c % 2].wait()
        for k in range(per):
            v = c * per + k
            row = v % 8 // 4 * half + (v // 8 + 1) * main + v % 4 * width
            buf[slot, :, k * LANES : (k + 1) * LANES] = full[row : row + width, :] * scale
        copy = pltpu.make_async_copy(buf.at[slot], out_ref.at[:, pl.ds(c * CHUNK, CHUNK)], sems.at[slot])
        copy.start()
        copies.append(copy)
    for c in (0, chunks):
        for copy in arrivals[c]:
            copy.wait()
    extra = half - EXTRA * UNIT
    side_copies = []
    for i, ref in enumerate((enc_ref, pred_ref)):
        for k in range(width // LANES):
            row = i * half + (k * width if k < 4 else extra)
            side_buf[i, :, k * LANES : (k + 1) * LANES] = full[row : row + width, :] * scale
        copy = pltpu.make_async_copy(side_buf.at[i], ref, sems.at[buf.shape[0] + i])
        copy.start()
        side_copies.append(copy)
    row = extra + width
    for k in range(vocab // LANES):
        bias_ref[:, k * LANES : (k + 1) * LANES] = full[row + k : row + k + 1, :] * scale
    row += vocab // LANES
    for k in range(width // LANES):
        joint_ref[:, k * LANES : (k + 1) * LANES] = full[row + k : row + k + 1, :] * scale
    row = half + extra + width
    loss = jnp.sum(full[row : row + 1, :], axis=1, keepdims=True)
    labels = jnp.sum(full[row + 1 : row + 2, :], axis=1, keepdims=True)
    loss_ref[...] = jnp.broadcast_to(loss / labels, loss_ref.shape)
    for copy in copies[-buf.shape[0] :] + side_copies:
        copy.wait()


def finish(full, squares, width, vocab, count):
    _, main, half = layout(width, vocab)
    vmem = pl.BlockSpec(memory_space=pltpu.VMEM)
    anywhere = pl.BlockSpec(memory_space=pl.ANY)
    shape = jax.ShapeDtypeStruct
    return pl.pallas_call(
        functools.partial(finish_kernel, main, half, float(count)),
        out_shape=(
            shape((width, vocab), F32), shape((width, width), F32), shape((width, width), F32),
            shape((1, vocab), F32), shape((1, width), F32), shape((1, LANES), F32),
        ),
        in_specs=[anywhere, vmem],
        out_specs=(anywhere, anywhere, anywhere, vmem, vmem, vmem),
        scratch_shapes=[
            pltpu.VMEM(full.shape, F32),
            pltpu.VMEM((4, width, CHUNK), F32),
            pltpu.VMEM((2, width, width), F32),
            pltpu.SemaphoreType.DMA((2, 2 + vocab // BLOCK)),
            pltpu.SemaphoreType.DMA((6,)),
        ],
        compiler_params=pltpu.CompilerParams(vmem_limit_bytes=63_000_000),
        name="finish",
    )(full, squares)


def per_device(enc, pred, labels, frame_len, label_len, w_enc, w_pred, b_joint, w_out, b_out):
    width, vocab = w_out.shape
    sums = local_grads(enc, pred, labels, frame_len, label_len, w_enc, w_pred, b_joint, w_out, b_out)
    full, squares = exchange(*sums)
    count = w_enc.size + w_pred.size + w_out.size + b_out.size + b_joint.size
    out, g_enc, g_pred, bias, joint, loss = finish(full, squares, width, vocab, count)
    return g_enc, g_pred, out, bias.reshape(vocab), joint.reshape(width), loss[0, 0]


def solution(mesh):
    split = P(AXES)
    in_specs = (split, split, split, split, split, P(), P(), P(), P(), P())
    return jax.shard_map(per_device, mesh=mesh, in_specs=in_specs, out_specs=(P(),) * 6, check_vma=False)
```

```python
import functools

import jax
import jax.numpy as jnp
from jax import lax
from jax.experimental import pallas as pl
from jax.experimental.pallas import tpu as pltpu
from jax.sharding import PartitionSpec as P

AXES = ("dp", "rep")
NEG = -1e30
EPS = 1e-06
F32 = jnp.float32
BF16 = jnp.bfloat16
LANES = 128
SLOT = 32
CHUNK = 512
ROWS = 416


def local_kernel(
    labels_ref, frame_ref, label_ref, enc_ref, pred_ref, w_enc_ref, w_pred_ref, b_joint_ref, w_out_hbm, b_out_ref,
    side_ref, dlog_ref, hid_t_ref,
    hid, hid_t, logits, dhid, dlog, top, tot, lse, occ, emit_occ, blank_occ, target, blank_d, emit_d, alpha_d,
    beta_d, below_d, right_d, pred_pad, dpred_pad, denc, bias_acc, slabs, tail, w_out_ref, b_joint_row, b_out_row, sems, side_sems, load_sem, hid_sem,
):
    utts, frames, _ = enc_ref.shape
    b_joint_row[...] = b_joint_ref[...].astype(F32).reshape(b_joint_row.shape)
    b_out_row[...] = b_out_ref[...].astype(F32).reshape(b_out_row.shape)
    slots = pred_ref.shape[1]
    width = w_enc_ref.shape[1]
    vocab = w_out_ref.shape[1]
    rows_all = hid.shape[0]
    load = pltpu.make_async_copy(w_out_hbm, w_out_ref, load_sem)
    load.start()
    cells = utts * slots * frames
    diags = frames + slots - 1
    blocks = [(i, u, (i * slots + u) * frames, SLOT * i + u) for i in range(utts) for u in range(slots)]
    lane_row = lax.broadcasted_iota(jnp.int32, (1, LANES), 1)
    lane_cell = lax.broadcasted_iota(jnp.int32, (frames, LANES), 1)

    def label_at(i, u):
        return labels_ref[i, u] if u < slots - 1 else 1

    pred_pad[...] = jnp.zeros_like(pred_pad)
    hid[cells:, :] = jnp.zeros((rows_all - cells, width), BF16)
    enc_proj = [jnp.dot(enc_ref[i], w_enc_ref[...], preferred_element_type=F32) for i in range(utts)]
    for i in range(utts):
        pred_pad[SLOT * i : SLOT * i + slots, :] = pred_ref[i]
    pred_proj = jnp.dot(pred_pad[...], w_pred_ref[...], preferred_element_type=F32) + b_joint_row[...]
    for i, u, row, col in blocks:
        hid[row : row + frames, :] = jnp.tanh(enc_proj[i] + pred_proj[col : col + 1, :]).astype(BF16)
    hid_t[...] = hid[...].T
    hid_copy = pltpu.make_async_copy(hid_t, hid_t_ref, hid_sem)
    hid_copy.start()
    load.wait()

    label_row = jnp.full((1, LANES), -1, jnp.int32)
    for i, u, row, col in blocks:
        label_row = jnp.where(lane_row == col, label_at(i, u), label_row)
    picks = lax.broadcasted_iota(jnp.int32, (vocab, LANES), 0) == label_row
    picks = picks.astype(F32).astype(BF16)
    w_pick = jnp.dot(w_out_ref[...], picks, preferred_element_type=F32).astype(BF16)
    b_pick = jnp.dot(
        jnp.broadcast_to(b_out_row[...], (16, vocab)).astype(BF16), picks, preferred_element_type=F32
    )[:1, :]
    w_blank = jnp.broadcast_to(w_out_ref[:, :1].astype(F32), (width, LANES)).astype(BF16)
    w_two = jnp.concatenate([w_pick, w_blank], axis=1)
    b_blank = b_out_row[:, :1]

    top[...] = jnp.full_like(top, NEG)
    tot[...] = jnp.zeros_like(tot)

    def forward(c, carry):
        cols = pl.ds(pl.multiple_of(c * CHUNK, CHUNK), CHUNK)
        w_c = w_out_ref[:, cols]
        b_c = b_out_row[:, cols]
        for r in range(0, rows_all, ROWS):
            z = jnp.dot(hid[r : r + ROWS, :], w_c, preferred_element_type=F32) + b_c
            logits[r : r + ROWS, cols] = z
            tiles = [z[:, k : k + LANES] for k in range(0, CHUNK, LANES)]
            old = top[r : r + ROWS, :]
            new = functools.reduce(jnp.maximum, tiles, old)
            top[r : r + ROWS, :] = new
            tot[r : r + ROWS, :] = tot[r : r + ROWS, :] * jnp.exp(old - new) + sum(jnp.exp(t - new) for t in tiles)
        return carry

    lax.fori_loop(0, vocab // CHUNK, forward, 0)

    for r in range(0, rows_all, ROWS):
        row_top = jnp.max(top[r : r + ROWS, :], axis=1, keepdims=True)
        row_sum = jnp.sum(tot[r : r + ROWS, :] * jnp.exp(top[r : r + ROWS, :] - row_top), axis=1, keepdims=True)
        row_lse = jnp.broadcast_to(row_top + jnp.log(row_sum), (ROWS, LANES))
        lse[r : r + ROWS, :] = row_lse
        two = jnp.dot(hid[r : r + ROWS, :], w_two, preferred_element_type=F32)
        top[r : r + ROWS, :] = two[:, :LANES] + b_pick - row_lse
        tot[r : r + ROWS, :] = two[:, LANES:] + b_blank - row_lse

    blank_d[...] = jnp.full_like(blank_d, NEG)
    emit_d[...] = jnp.full_like(emit_d, NEG)
    for i, u, row, col in blocks:
        here = lane_cell == col
        emit_d[u : u + frames, :] = jnp.where(here, top[row : row + frames, :], emit_d[u : u + frames, :])
        blank_d[u : u + frames, :] = jnp.where(here, tot[row : row + frames, :], blank_d[u : u + frames, :])
    label_pos = lax.rem(lane_row, SLOT)
    frame_count = jnp.full((1, LANES), 0, jnp.int32)
    label_count = jnp.full((1, LANES), -1, jnp.int32)
    for i in range(utts):
        mine = lane_row // SLOT == i
        frame_count = jnp.where(mine, frame_ref[i], frame_count)
        label_count = jnp.where(mine, label_ref[i], label_count)

    def join(a, b):
        hi = jnp.maximum(a, b)
        return hi + jnp.log(1.0 + jnp.exp(jnp.minimum(a, b) - hi))

    alpha = jnp.where((label_pos == 0) & (lane_row < SLOT * utts), 0.0, NEG).astype(F32)
    beta = jnp.full((1, LANES), NEG, F32)
    alpha_d[0:1, :] = alpha
    for step in range(diags):
        d = diags - 1 - step
        t = d - label_pos
        live = (t >= 0) & (t < frame_count) & (label_pos <= label_count)
        last = (t == frame_count - 1) & (label_pos == label_count)
        below = jnp.where(last, 0.0, beta)
        right = pltpu.roll(beta, LANES - 1, 1)
        below_d[d : d + 1, :] = below
        right_d[d : d + 1, :] = right
        beta = jnp.where(live, join(below + blank_d[d : d + 1, :], right + emit_d[d : d + 1, :]), NEG)
        beta_d[d : d + 1, :] = beta
        if step > 0:
            left = pltpu.roll(alpha + emit_d[step - 1 : step, :], 1, 1)
            alpha = join(alpha + blank_d[step - 1 : step, :], left)
            alpha_d[step : step + 1, :] = alpha
    total = jnp.full((1, LANES), 0.0, F32)
    for i in range(utts):
        beta_0 = jnp.sum(jnp.where(lane_row == SLOT * i, beta, 0.0), axis=1, keepdims=True)
        total = jnp.where(lane_row // SLOT == i, beta_0, total)
    span = slice(0, diags)
    blank_d[span, :] = jnp.exp(
        jnp.minimum(alpha_d[span, :] + blank_d[span, :] + below_d[span, :] - total, 80.0)
    )
    emit_d[span, :] = jnp.exp(jnp.minimum(alpha_d[span, :] + emit_d[span, :] + right_d[span, :] - total, 80.0))

    pad = slice(cells, rows_all)
    occ[pad, :] = jnp.zeros((rows_all - cells, LANES), F32)
    emit_occ[pad, :] = jnp.zeros((rows_all - cells, LANES), F32)
    blank_occ[pad, :] = jnp.zeros((rows_all - cells, LANES), F32)
    target[pad, :] = jnp.full((rows_all - cells, LANES), -1, jnp.int32)
    for i, u, row, col in blocks:
        here = slice(row, row + frames)
        b = jnp.broadcast_to(blank_d[u : u + frames, col : col + 1], (frames, LANES))
        e = jnp.broadcast_to(emit_d[u : u + frames, col : col + 1], (frames, LANES))
        blank_occ[here, :] = b
        emit_occ[here, :] = e
        occ[here, :] = b + e
        target[here, :] = jnp.full((frames, LANES), label_at(i, u), jnp.int32)

    dhid[...] = jnp.zeros_like(dhid)

    bias_acc[...] = jnp.zeros_like(bias_acc)

    def out_copy(c, slot):
        cols = pl.ds(pl.multiple_of(c * CHUNK, CHUNK), CHUNK)
        return pltpu.make_async_copy(dlog.at[slot], dlog_ref.at[:, cols], sems.at[slot])

    def backward(c, carry):
        cols = pl.ds(pl.multiple_of(c * CHUNK, CHUNK), CHUNK)
        slot = lax.rem(c, 2)
        w_c = w_out_ref[:, cols]
        first = c == 0

        @pl.when(c >= 2)
        def _():
            out_copy(c - 2, slot).wait()

        sums = [jnp.zeros((8, LANES), F32)] * (CHUNK // LANES)
        for r in range(0, rows_all, ROWS):
            here = slice(r, r + ROWS)
            row_lse, row_occ, row_emit = lse[here, :], occ[here, :], emit_occ[here, :]
            row_target = target[here, :] - c * CHUNK
            lane = lax.broadcasted_iota(jnp.int32, (ROWS, LANES), 1)
            parts = []
            for k in range(0, CHUNK, LANES):
                z = logits[here, pl.ds(pl.multiple_of(c * CHUNK + k, LANES), LANES)]
                d = jnp.exp(z - row_lse) * row_occ - jnp.where(lane + k == row_target, row_emit, 0.0)
                if k == 0:
                    d = d - jnp.where((lane == 0) & first, blank_occ[here, :], 0.0)
                sums[k // LANES] = sums[k // LANES] + jnp.sum(d.reshape(ROWS // 8, 8, LANES), axis=0)
                parts.append(d.astype(BF16))
            d = jnp.concatenate(parts, axis=1)
            dlog[slot, here, :] = d
            dhid[here, :] += lax.dot_general(d, w_c, (((1,), (1,)), ((), ())), preferred_element_type=F32)
        bias_acc[:, cols] = jnp.concatenate(sums, axis=1)
        out_copy(c, slot).start()
        return carry

    steps = vocab // CHUNK
    lax.fori_loop(0, steps, backward, 0)

    dpred_pad[...] = jnp.zeros_like(dpred_pad)
    for i in range(utts):
        enc_sum = jnp.zeros((frames, width), F32)
        for u in range(slots):
            row = (i * slots + u) * frames
            h = hid[row : row + frames, :].astype(F32)
            dpre = dhid[row : row + frames, :] * (1.0 - h * h)
            enc_sum = enc_sum + dpre
            dpred_pad[SLOT * i + u : SLOT * i + u + 1, :] = jnp.sum(dpre, axis=0, keepdims=True)
        denc[i] = enc_sum.astype(BF16)
    dpred = dpred_pad[...].astype(BF16)
    over_rows = (((0,), (0,)), ((), ()))
    g_enc = jnp.zeros((width, width), F32)
    for i in range(utts):
        g_enc = g_enc + lax.dot_general(enc_ref[i], denc[i], over_rows, preferred_element_type=F32)
    g_pred = lax.dot_general(pred_pad[...], dpred, over_rows, preferred_element_type=F32)
    per = width // LANES
    last_copies = []
    for i, g in enumerate((g_enc, g_pred)):
        for k in range(per):
            slabs[i, k] = g[:, k * LANES : (k + 1) * LANES]
        for k in range(per):
            last_copies.append(
                pltpu.make_async_copy(slabs.at[i, k], side_ref.at[i, pl.ds(k * width, width), :], side_sems.at[i, k])
            )
            last_copies[-1].start()
    tail[...] = jnp.zeros_like(tail)
    bias = jnp.sum(bias_acc[...], axis=0, keepdims=True)
    joint = jnp.sum(dpred.astype(F32), axis=0, keepdims=True)
    for k in range(vocab // LANES):
        tail[0, k : k + 1, :] = bias[:, k * LANES : (k + 1) * LANES]
    for k in range(per):
        tail[0, vocab // LANES + k : vocab // LANES + k + 1, :] = joint[:, k * LANES : (k + 1) * LANES]
    head = (lax.rem(lane_row, SLOT) == 0) & (lane_row < SLOT * utts)
    tail[1, 0:1, :] = jnp.where(head, -beta_d[0:1, :], 0.0)
    tail[1, 1:2, :] = jnp.where(head, label_count.astype(F32), 0.0)
    for i in range(2):
        last_copies.append(
            pltpu.make_async_copy(
                tail.at[i], side_ref.at[i, pl.ds(per * width, tail.shape[1]), :], side_sems.at[i, per]
            )
        )
        last_copies[-1].start()
    for c in range(max(0, steps - 2), steps):
        out_copy(c, c % 2).wait()
    hid_copy.wait()
    for copy in last_copies:
        copy.wait()


UNIT = 512
PER_CHUNK = 5
BLOCK = 1024
GAP = 2
GROUPS = ((0,), (1,), (2, 3), (4, 5))
EXTRA = 2


def layout(width, vocab):
    chunks = 1 + vocab // BLOCK
    main = PER_CHUNK * UNIT
    half = chunks * main + EXTRA * UNIT
    per = width // LANES
    assert main == 4 * width and BLOCK == 8 * LANES and per == 5
    return chunks, main, half


def local_grads(enc, pred, labels, frame_len, label_len, w_enc, w_pred, b_joint, w_out, b_out):
    utts, frames, enc_dim = enc.shape
    slots, pred_dim = pred.shape[1:]
    width, vocab = w_out.shape
    rows_all = -(-utts * slots * frames // ROWS) * ROWS
    diags = frames + slots
    diag_rows = -(-diags // 8) * 8
    chunks, main, half = layout(width, vocab)
    side_rows = main + EXTRA * UNIT
    shape = jax.ShapeDtypeStruct
    smem = pl.BlockSpec(memory_space=pltpu.SMEM)
    vmem = pl.BlockSpec(memory_space=pltpu.VMEM)
    anywhere = pl.BlockSpec(memory_space=pl.ANY)
    cell = lambda t: pltpu.VMEM((rows_all, LANES), t)
    diag = pltpu.VMEM((diag_rows, LANES), F32)
    return pl.pallas_call(
        local_kernel,
        out_shape=(
            shape((2, side_rows, LANES), F32), shape((rows_all, vocab), BF16), shape((width, rows_all), BF16),
        ),
        in_specs=[smem] * 3 + [vmem] * 5 + [anywhere, vmem],
        out_specs=(anywhere,) * 3,
        scratch_shapes=[
            pltpu.VMEM((rows_all, width), BF16),
            pltpu.VMEM((width, rows_all), BF16),
            pltpu.VMEM((rows_all, vocab), F32),
            pltpu.VMEM((rows_all, width), F32),
            pltpu.VMEM((2, rows_all, CHUNK), BF16),
            cell(F32), cell(F32), cell(F32), cell(F32), cell(F32), cell(F32), cell(jnp.int32),
            diag, diag, diag, diag, diag, diag,
            pltpu.VMEM((SLOT * utts, pred_dim), BF16),
            pltpu.VMEM((SLOT * utts, width), F32),
            pltpu.VMEM((utts, frames, width), BF16),
            pltpu.VMEM((8, vocab), F32),
            pltpu.VMEM((2, width // LANES, width, LANES), F32),
            pltpu.VMEM((2, side_rows - width // LANES * width, LANES), F32),
            pltpu.VMEM((width, vocab), BF16),
            pltpu.VMEM((1, width), F32),
            pltpu.VMEM((1, vocab), F32),
            pltpu.SemaphoreType.DMA((2,)),
            pltpu.SemaphoreType.DMA((2, width // LANES + 1)),
            pltpu.SemaphoreType.DMA(()),
            pltpu.SemaphoreType.DMA(()),
        ],
        compiler_params=pltpu.CompilerParams(vmem_limit_bytes=66_000_000),
        name="local_grads",
    )(labels, frame_len, label_len, enc, pred, w_enc, w_pred, b_joint, w_out, b_out)


def exchange_kernel(
    chunks, side_ref, dlog_ref, hid_t_ref, full_ref, squares_ref, full, held, from_core, arrived, d_buf, total_ref,
    out_sems, side_sems, d_sems, core_sems, step_sems, extra_sems,
):
    dp, x = lax.axis_index("dp"), lax.axis_index("rep")
    core = lax.rem(dp, 2)
    place = (x, dp // 8, lax.rem(dp // 2, 4))
    width = hid_t_ref.shape[0]
    extra_at = chunks * PER_CHUNK

    def device(x, y, z, core):
        return ((y * 4 + z) * 2 + core, x)

    other_core = device(*place, 1 - core)

    def link(turn, s):
        axis = (turn + s) % 3
        v = place[axis]
        second = lax.rem((turn + s) // 3 + core, 2)
        peer = second * (3 - v) + (1 - second) * (v + 1 - 2 * lax.rem(v, 2))
        bit = second * (v // 2) + (1 - second) * lax.rem((v + 1) // 2, 2)
        return axis, peer, bit

    def peers_of(turn, group):
        found = []
        for mask in range(1, 1 << len(group)):
            flips = [i for i in range(len(group)) if mask >> i & 1]
            where = list(place)
            for i in flips:
                axis, peer, _ = link(turn, group[i])
                where[axis] = peer
            found.append((flips, device(*where, core)))
        return found

    turns = list(range(PER_CHUNK)) + [5, 2]
    bits = [[link(turn, s)[2] for s in range(6)] for turn in turns]
    barrier = pltpu.get_barrier_semaphore()
    greeted = {}
    for turn in range(6):
        for group in GROUPS:
            for flips, peer in peers_of(turn, group):
                key = frozenset((turn + group[i]) % 6 for i in flips)
                greeted[key] = peer
    peers = [other_core] + list(greeted.values())
    for peer in peers:
        pl.semaphore_signal(barrier, inc=1, device_id=peer, device_id_type=pl.DeviceIdType.MESH)

    side_copies = []
    for h in range(2):
        for n, (src, dst, units) in enumerate(((0, 0, PER_CHUNK), (PER_CHUNK, extra_at, EXTRA))):
            copy = pltpu.make_async_copy(
                side_ref.at[h, pl.ds(src, units)], held.at[h, pl.ds(dst, units)], side_sems.at[h, n]
            )
            copy.start()
            side_copies.append(copy)

    def load_block(c):
        slot = lax.rem(c, 2)
        cols = pl.ds(pl.multiple_of((c - 1) * BLOCK, BLOCK), BLOCK)
        return pltpu.make_async_copy(dlog_ref.at[:, cols], d_buf.at[slot], d_sems.at[slot])

    load_block(1).start()

    offsets = []
    for line_bits in bits:
        line = [0]
        for s in range(6):
            line.append(line[-1] + line_bits[s] * (UNIT >> (s + 1)))
        offsets.append(line)

    def rows(start, n):
        return pl.ds(pl.multiple_of(start, 8), n)

    def remote(src, dst, sems, index, peer):
        return pltpu.make_async_remote_copy(
            src_ref=src, dst_ref=dst, send_sem=sems.at[(*index, 0)], recv_sem=sems.at[(*index, 1)],
            device_id=peer, device_id_type=pl.DeviceIdType.MESH,
        )

    def unit_of(c, j):
        return c * PER_CHUNK + j if j < PER_CHUNK else extra_at + j - PER_CHUNK

    def sem_of(c, j, n):
        return (step_sems, (c, j, n)) if j < PER_CHUNK else (extra_sems, (j - PER_CHUNK, n))

    def swap(c, extra):
        units = pl.ds(extra_at, EXTRA) if extra else pl.ds(c * PER_CHUNK, PER_CHUNK)
        return remote(
            held.at[1 - core, units], from_core.at[units], core_sems, (chunks if extra else c,), other_core
        )

    lands, numbers = [], []
    at = number = 0
    for group in GROUPS:
        count = (1 << len(group)) - 1
        lands.append(at)
        numbers.append(number)
        at += count * (UNIT >> (group[-1] + 1))
        number += count
    per_way = number

    def reduce(c, j, g):
        group = GROUPS[g]
        n = UNIT >> (group[-1] + 1)
        u = unit_of(c, j)
        copies = []
        for m, (flips, peer) in enumerate(peers_of(turns[j], group)):
            start = offsets[j][group[0]]
            for i, s in enumerate(group):
                bit = bits[j][s]
                start = start + (1 - bit if i in flips else bit) * (UNIT >> (s + 1))
            copies.append(
                remote(
                    held.at[core, u, rows(start, n)], arrived.at[u, pl.ds(lands[g] + m * n, n)],
                    *sem_of(c, j, numbers[g] + m), peer,
                )
            )
        return copies

    def add_reduce(c, j, g):
        group = GROUPS[g]
        n = UNIT >> (group[-1] + 1)
        u = unit_of(c, j)
        here = rows(offsets[j][group[-1] + 1], n)
        total = held[core, u, here, :]
        for m in range((1 << len(group)) - 1):
            total = total + arrived[u, pl.ds(lands[g] + m * n, n), :]
        if g < len(GROUPS) - 1:
            held[core, u, here, :] = total
        else:
            full[core, u, here, :] = total

    def gather(c, j, g):
        group = GROUPS[g]
        here = full.at[core, unit_of(c, j), rows(offsets[j][group[-1] + 1], UNIT >> (group[-1] + 1))]
        return [
            remote(here, here, *sem_of(c, j, per_way + numbers[g] + m), peer)
            for m, (_, peer) in enumerate(peers_of(turns[j], group))
        ]

    def give(c, j, late):
        n = UNIT // 2
        bit = bits[j][0]
        start = (1 - bit) * n if late else bit * n
        here = full.at[core, unit_of(c, j), rows(start, n)]
        return [remote(here, here, *sem_of(c, j, 2 * per_way + late), other_core)]

    def put(c, extra):
        units = pl.ds(extra_at, EXTRA) if extra else pl.ds(c * PER_CHUNK, PER_CHUNK)
        return [
            pltpu.make_async_copy(full.at[h, units], full_ref.at[h, units], out_sems.at[chunks if extra else c, h])
            for h in range(2)
        ]

    def start(copies):
        for copy in copies:
            copy.start()

    def wait(copies):
        for copy in copies:
            copy.wait()

    lines = 64

    def add_squares(here):
        here = here.reshape(here.shape[0] // lines, lines, LANES)
        total_ref[...] = total_ref[...] + jnp.sum(here * here, axis=0)

    last = len(GROUPS) - 1

    def stage(k, c, lanes):
        extra = lanes[0] >= PER_CHUNK
        if k == 1:
            swap(c, extra).wait()
            units = pl.ds(extra_at, EXTRA) if extra else pl.ds(c * PER_CHUNK, PER_CHUNK)
            held[core, units] = held[core, units] + from_core[units]
            for j in lanes:
                start(reduce(c, j, 0))
        elif k <= last + 2:
            for j in lanes:
                wait(reduce(c, j, k - 2))
                add_reduce(c, j, k - 2)
            for j in lanes:
                start(reduce(c, j, k - 1) if k <= last + 1 else gather(c, j, last))
        elif k <= 2 * last + 2:
            g = 2 * last + 2 - k
            for j in lanes:
                wait(gather(c, j, g + 1))
                start(gather(c, j, g))
                if g == 0:
                    start(give(c, j, 0))
        elif k == 2 * last + 3:
            for j in lanes:
                wait(gather(c, j, 0))
                start(give(c, j, 1))
        else:
            for j in lanes:
                wait(give(c, j, 0))
                wait(give(c, j, 1))
            start(put(c, extra))
            for h in range(2):
                if extra:
                    left = width - UNIT if h else EXTRA * UNIT - UNIT
                    add_squares(full[h, extra_at])
                    add_squares(full[h, extra_at + 1, 0:left, :])
                else:
                    for j in lanes:
                        add_squares(full[h, unit_of(c, j)])

    stages = 2 * last + 4
    total_ref[...] = jnp.zeros_like(total_ref)
    pl.semaphore_wait(barrier, len(peers))

    def tick(t, carry):
        for k in range(1, stages + 1):

            @pl.when((t >= GAP * k) & (t < chunks + GAP * k))
            def _(k=k):
                stage(k, t - GAP * k, range(PER_CHUNK))

            @pl.when(t == GAP * k)
            def _(k=k):
                stage(k, 0, range(PER_CHUNK, PER_CHUNK + EXTRA))

        @pl.when(t == 0)
        def _():
            for copy in side_copies:
                copy.wait()
            swap(0, False).start()
            swap(0, True).start()

        @pl.when((t >= 1) & (t < chunks))
        def _():
            load_block(t).wait()

            @pl.when(t + 1 < chunks)
            def _():
                load_block(t + 1).start()

            slot = lax.rem(t, 2)
            for h in range(2):
                g = jnp.dot(
                    hid_t_ref[...], d_buf[slot, :, h * BLOCK // 2 : (h + 1) * BLOCK // 2], preferred_element_type=F32
                )
                tiles = jnp.concatenate([g[:, k * LANES : (k + 1) * LANES] for k in range(4)], axis=0)
                held[h, pl.ds(t * PER_CHUNK, PER_CHUNK)] = tiles.reshape(PER_CHUNK, UNIT, LANES)
            swap(t, False).start()

        return carry

    lax.fori_loop(0, chunks + GAP * stages, tick, 0)

    squares_ref[...] = jnp.sum(total_ref[...].reshape(lines // 8, 8, LANES), axis=0)
    for c in range(chunks):
        wait(put(c, False))
    wait(put(0, True))


def exchange(side, dlog, hid_t):
    width, rows_all = hid_t.shape
    vocab = dlog.shape[1]
    chunks, main, half = layout(width, vocab)
    units = half // UNIT
    messages = 2 * sum((1 << len(group)) - 1 for group in GROUPS) + 2
    vmem = pl.BlockSpec(memory_space=pltpu.VMEM)
    anywhere = pl.BlockSpec(memory_space=pl.ANY)
    shape = jax.ShapeDtypeStruct
    full, squares = pl.pallas_call(
        functools.partial(exchange_kernel, chunks),
        out_shape=(shape((2, units, UNIT, LANES), F32), shape((8, LANES), F32)),
        in_specs=[anywhere, anywhere, vmem],
        out_specs=(anywhere, vmem),
        scratch_shapes=[
            pltpu.VMEM((2, units, UNIT, LANES), F32),
            pltpu.VMEM((2, units, UNIT, LANES), F32),
            pltpu.VMEM((units, UNIT, LANES), F32),
            pltpu.VMEM((units, UNIT, LANES), F32),
            pltpu.VMEM((2, rows_all, BLOCK), BF16),
            pltpu.VMEM((64, LANES), F32),
            pltpu.SemaphoreType.DMA((chunks + 1, 2)),
            pltpu.SemaphoreType.DMA((2, 2)),
            pltpu.SemaphoreType.DMA((2,)),
            pltpu.SemaphoreType.DMA((chunks + 1, 2)),
            pltpu.SemaphoreType.DMA((chunks, PER_CHUNK, messages, 2)),
            pltpu.SemaphoreType.DMA((EXTRA, messages, 2)),
        ],
        compiler_params=pltpu.CompilerParams(collective_id=0, has_side_effects=True, vmem_limit_bytes=63_000_000),
        name="exchange",
    )(side.reshape(2, side.shape[1] // UNIT, UNIT, LANES), dlog, hid_t)
    return full.reshape(2 * half, LANES), squares


def finish_kernel(main, half, count, full, squares_ref, out_ref, enc_ref, pred_ref, bias_ref, joint_ref, loss_ref, buf, side_buf, sems):
    width, vocab = out_ref.shape
    squares = jnp.sum(jnp.sum(squares_ref[...], axis=0, keepdims=True), axis=1, keepdims=True)
    scale = lax.rsqrt(squares * (1.0 / count) + EPS)
    copies = []
    steps = vocab // CHUNK
    per = CHUNK // LANES
    for c in range(steps):
        slot = c % buf.shape[0]
        if c >= buf.shape[0]:
            copies[c - buf.shape[0]].wait()
        for k in range(per):
            v = c * per + k
            row = v % 8 // 4 * half + (v // 8 + 1) * main + v % 4 * width
            buf[slot, :, k * LANES : (k + 1) * LANES] = full[row : row + width, :] * scale
        copy = pltpu.make_async_copy(buf.at[slot], out_ref.at[:, pl.ds(c * CHUNK, CHUNK)], sems.at[slot])
        copy.start()
        copies.append(copy)
    extra = half - EXTRA * UNIT
    side_copies = []
    for i, ref in enumerate((enc_ref, pred_ref)):
        for k in range(width // LANES):
            row = i * half + (k * width if k < 4 else extra)
            side_buf[i, :, k * LANES : (k + 1) * LANES] = full[row : row + width, :] * scale
        copy = pltpu.make_async_copy(side_buf.at[i], ref, sems.at[buf.shape[0] + i])
        copy.start()
        side_copies.append(copy)
    row = extra + width
    for k in range(vocab // LANES):
        bias_ref[:, k * LANES : (k + 1) * LANES] = full[row + k : row + k + 1, :] * scale
    row += vocab // LANES
    for k in range(width // LANES):
        joint_ref[:, k * LANES : (k + 1) * LANES] = full[row + k : row + k + 1, :] * scale
    row = half + extra + width
    loss = jnp.sum(full[row : row + 1, :], axis=1, keepdims=True)
    labels = jnp.sum(full[row + 1 : row + 2, :], axis=1, keepdims=True)
    loss_ref[0, 0] = jnp.sum(loss / labels)
    for copy in copies[-buf.shape[0] :] + side_copies:
        copy.wait()


def finish(full, squares, width, vocab, count):
    _, main, half = layout(width, vocab)
    vmem = pl.BlockSpec(memory_space=pltpu.VMEM)
    anywhere = pl.BlockSpec(memory_space=pl.ANY)
    shape = jax.ShapeDtypeStruct
    return pl.pallas_call(
        functools.partial(finish_kernel, main, half, float(count)),
        out_shape=(
            shape((width, vocab), F32), shape((width, width), F32), shape((width, width), F32),
            shape((1, vocab), F32), shape((1, width), F32), shape((1, 1), F32),
        ),
        in_specs=[vmem, vmem],
        out_specs=(anywhere, anywhere, anywhere, vmem, vmem, pl.BlockSpec(memory_space=pltpu.SMEM)),
        scratch_shapes=[
            pltpu.VMEM((4, width, CHUNK), F32),
            pltpu.VMEM((2, width, width), F32),
            pltpu.SemaphoreType.DMA((6,)),
        ],
        compiler_params=pltpu.CompilerParams(vmem_limit_bytes=40_000_000),
        name="finish",
    )(full, squares)


def per_device(enc, pred, labels, frame_len, label_len, w_enc, w_pred, b_joint, w_out, b_out):
    width, vocab = w_out.shape
    sums = local_grads(enc, pred, labels, frame_len, label_len, w_enc, w_pred, b_joint, w_out, b_out)
    full, squares = exchange(*sums)
    count = w_enc.size + w_pred.size + w_out.size + b_out.size + b_joint.size
    out, g_enc, g_pred, bias, joint, loss = finish(full, squares, width, vocab, count)
    return g_enc, g_pred, out, bias.reshape(vocab), joint.reshape(width), loss.reshape(())


def solution(mesh):
    split = P(AXES)
    in_specs = (split, split, split, split, split, P(), P(), P(), P(), P())
    return jax.shard_map(per_device, mesh=mesh, in_specs=in_specs, out_specs=(P(),) * 6, check_vma=False)
```
